256 devices in a mesh: sims: 4 (over z_hi, core), blk: 64 (over x, z_lo, y).
Axes of the slice: x: 4, y: 4, z: 8 (z_hi: 2, z_lo: 4; z = z_hi * 4 + z_lo), core: 2. Of those that a mesh axis runs over, the one named last changes fastest.
Arguments:
- sim_alm: bfloat16 [1536, 16, 2, 1536], P('blk', 'sims'), may hold values from -6 to 6
- t_filter: float32 [1536], replicated, may hold values from 0.0006510417 to 0.00390625
- wiener_filter: float32 [1536], replicated, may hold values from 8.477105e-07 to 5.086263e-06
- colatitude: float32 [128], replicated, may hold values from 1.09712 to 1.60288, as said below
- legendre: bfloat16 [1536, 1536, 128], P('blk'), may hold values from -2 to 2, as said below
- pixel_mask: int32 [128, 4096], P('blk'), may hold values 0 or 1
Outputs:
- field_sum: float32 [1536, 2, 1536], P('blk', None, 'sims')
- spectra: float32 [16, 2, 1536], P('sims')
The draws below stay inside these ranges and needn't reach their ends.
Inputs may be any that keep to these rules, and one draw needn't show every extreme that they name: `colatitude`: the colatitudes of 128 cycles in increasing order, about 0.0016 apart, in a band centred between 1.2 and 1.5. legendre[m,l,r] is the orthonormal associated Legendre function of degree l and order m at colatitude[r], zero for l < m, rounded to bfloat16.
All inputs are finite; a program needn't handle non-finite values. No bound on the sum of `pixel_mask` on one device may be relied on, other than what follows from the above.
Results may differ from the reference program's by a relative error of at most 0.006.
The reference program's roundings to bfloat16 on the way (of `coefs`, `cycle_coefs`, `fourier`, `flow_maps`, `mode_coefs` and `tilted`) count: a program that leaves them out, or rounds other values in their place, can miss the bound.
Values may be sent and summed in bfloat16 or wider, within the bound.
No kernel may reach another device: no remote copies, remote signals or barrier semaphores. Data moves between devices by JAX's collectives and lax.ppermute only.
A program may use at most 192 MiB of HBM per device.

```python
import math
import jax
import jax.numpy as jnp
from jax import lax

L = 1536
NPHI = 4096
CYCLES = 128
NSIM = 16


def cycle_angles(key):
    jitter = jax.random.uniform(jax.random.fold_in(key, 11), (CYCLES,), jnp.float32, -0.3, 0.3)
    center = jax.random.uniform(jax.random.fold_in(key, 17), (), jnp.float32, 1.2, 1.5)
    spacing = jnp.arange(CYCLES, dtype=jnp.float32) + 0.5 - CYCLES / 2.0 + jitter
    return center + 0.0016 * spacing


def draw_colatitude(key, part):
    return cycle_angles(key)


def draw_legendre(key, part):
    angles = cycle_angles(key)
    cosine = jnp.cos(angles)[None, :]
    log_sine = jnp.log(jnp.sin(angles))[None, :]
    orders = jnp.arange(L, dtype=jnp.float32)[:, None]
    counting = jnp.arange(1, L, dtype=jnp.float32)
    halves = jnp.log((2.0 * counting - 1.0) / (2.0 * counting))
    running = jnp.concatenate([jnp.zeros((1,), jnp.float32), jnp.cumsum(halves)])[:, None]
    diagonal = jnp.exp(0.5 * jnp.log((2.0 * orders + 1.0) / (4.0 * math.pi)) + 0.5 * running + orders * log_sine)

    def advance(state_pair, degree):
        previous, older = state_pair
        ratio_now = jnp.sqrt(jnp.maximum(4.0 * degree * degree - 1.0, 1.0) / jnp.maximum(degree * degree - orders * orders, 1.0))
        lower_degree = degree - 1.0
        ratio_before = jnp.sqrt(jnp.maximum(4.0 * lower_degree * lower_degree - 1.0, 1.0) / jnp.maximum(lower_degree * lower_degree - orders * orders, 1.0))
        general = ratio_now * (cosine * previous - older / ratio_before)
        current = jnp.where(degree == orders, diagonal, jnp.where(degree > orders, general, 0.0))
        return ((current, previous), current.astype(jnp.bfloat16))
    start = jnp.zeros((L, CYCLES), jnp.float32)
    final_state, stacked_rows = lax.scan(advance, (start, start), jnp.arange(L, dtype=jnp.float32))
    return jnp.transpose(stacked_rows, (1, 0, 2))


def with_ends(values, key, low, high):
    longest = values.shape.index(max(values.shape))
    spots = []
    for shift in (0, 1):
        where = [jax.random.randint(jax.random.fold_in(key, axis), (), 0, length) for axis, length in enumerate(values.shape)]
        where[longest] = (where[longest] + shift) % values.shape[longest]
        spots.append(tuple(where))
    return values.at[spots[0]].set(low).at[spots[1]].set(high)


def steps_of(rng, dims, shards, smallest, top_value):
    factor_of = 1.0
    for dim, shards_of in shards:
        steps = jax.random.uniform(jax.random.fold_in(jax.random.fold_in(rng, 6), dim), (shards_of,), jnp.float32, smallest / len(shards), top_value / len(shards))
        factor_of = factor_of * jnp.repeat(jnp.exp(steps), dims[dim] // shards_of).reshape((-1,) + (1,) * (len(dims) - 1 - dim))
    return factor_of


def scatter_about(stream_key, shape, deviation, most, cuts=(), kind=jnp.bfloat16):
    drawn = deviation * jax.random.normal(stream_key, shape, jnp.float32)
    if cuts:
        drawn = drawn * steps_of(stream_key, shape, cuts, -0.22, 0.18)
    return jnp.clip(drawn, -most, most).astype(kind)


def setup_inputs(seed: int = 0) -> dict:
    splits = jax.random.split(jax.random.key(seed), 7)
    sim_alm = scatter_about(splits[0], (L, NSIM, 2, L), 1.0, 6.0, ((0, 64), (1, 4)))
    t_filter = jnp.clip(jnp.exp(jax.random.uniform(splits[1], (L,), jnp.float32, math.log(0.0006510417), math.log(0.00390625))), 0.0006510417, 0.00390625)
    wiener_filter = jnp.clip(jnp.exp(jax.random.uniform(splits[2], (L,), jnp.float32, math.log(8.477105097881577e-07), math.log(5.086263172415784e-06))), 8.477105097881577e-07, 5.086263172415784e-06)
    colatitude = draw_colatitude(jax.random.fold_in(splits[6], 71), 0)
    legendre = draw_legendre(jax.random.fold_in(splits[6], 71), 0)
    pixel_mask = with_ends((jax.random.randint(splits[5], (CYCLES, NPHI), 0, 5) < 4).astype(jnp.int32), jax.random.fold_in(splits[5], 1), 0, 1)
    return {"sim_alm": sim_alm, "t_filter": t_filter, "wiener_filter": wiener_filter, "colatitude": colatitude, "legendre": legendre, "pixel_mask": pixel_mask}


def ladder(degree, orders):
    numerator = (2.0 * degree + 1.0) * (degree * degree - orders * orders)
    denominator = jnp.maximum(2.0 * degree - 1.0, 1.0)
    return jnp.where(degree > orders, jnp.sqrt(jnp.maximum(numerator, 0.0) / denominator), 0.0)

def fourier_table(mode_count, pixels):
    mode_ids = jnp.arange(mode_count, dtype=jnp.int32)[:, None]
    pixel_ids = jnp.arange(pixels, dtype=jnp.int32)[None, :]
    phases = 2.0 * math.pi / pixels * (mode_ids * pixel_ids % pixels).astype(jnp.float32)
    return jnp.stack([jnp.cos(phases).astype(jnp.bfloat16), (-jnp.sin(phases)).astype(jnp.bfloat16)], axis=1)

def reference(sim_alm, t_filter, wiener_filter, colatitude, legendre, pixel_mask):
    highest = lax.Precision.HIGHEST
    degree = jnp.arange(L, dtype=jnp.float32)
    orders = jnp.arange(L, dtype=jnp.float32)
    ladder_steps = ladder(degree[None, :], orders[:, None])
    lookup = legendre.astype(jnp.float32)
    fourier = fourier_table(L, NPHI).astype(jnp.float32)
    mode_weight = jnp.where(orders > 0, 2.0, 1.0)
    mode_weight_half = mode_weight.astype(jnp.bfloat16)
    cotangent = jnp.cos(colatitude) / jnp.sin(colatitude)
    cosecant = 1.0 / jnp.sin(colatitude)
    tilt_factor = jnp.cos(colatitude)
    pixel_weight = pixel_mask.astype(jnp.float32)

    def one_sim(coefficients):
        values = coefficients.astype(jnp.float32)
        weighted = wiener_filter * values
        raised = ladder_steps[:, None, :] * weighted
        lowered = jnp.concatenate([raised[..., 1:], jnp.zeros_like(raised[..., :1])], axis=-1)
        coefs = jnp.stack([t_filter * values, weighted, degree * weighted, lowered], axis=1).astype(jnp.bfloat16)
        legsum = jnp.einsum('mkcl,mlr->mkcr', coefs.astype(jnp.float32), lookup, precision=highest)
        rotated = jnp.stack([-legsum[:, 1, 1], legsum[:, 1, 0]], axis=1) * (orders[:, None, None] * cosecant)
        slopes = cotangent * legsum[:, 2] - cosecant * legsum[:, 3]
        cycle_coefs = jnp.stack([legsum[:, 0], rotated, slopes], axis=1).astype(jnp.bfloat16)
        scaled = cycle_coefs * mode_weight_half[:, None, None, None]
        cycle_maps = jnp.einsum('mqcr,mcj->qrj', scaled.astype(jnp.float32), fourier, precision=highest)
        product = pixel_weight * cycle_maps[0]
        flow_maps = jnp.stack([product * cycle_maps[2], product * cycle_maps[1]]).astype(jnp.bfloat16)
        mode_coefs = (jnp.einsum('prj,mcj->mpcr', flow_maps.astype(jnp.float32), fourier, precision=highest) * (2.0 * math.pi / NPHI)).astype(jnp.bfloat16)
        tilted = (tilt_factor * mode_coefs[:, 0].astype(jnp.float32)).astype(jnp.bfloat16)
        stacked = jnp.stack([tilted, mode_coefs[:, 0], mode_coefs[:, 1]], axis=1)
        projected = jnp.einsum('mkcr,mlr->mkcl', stacked.astype(jnp.float32), lookup, precision=highest)
        shifted = jnp.concatenate([jnp.zeros_like(projected[:, 1, :, :1]), projected[:, 1, :, :-1]], axis=-1)
        real_part = degree * projected[:, 0, 0] - ladder_steps * shifted[:, 0] + orders[:, None] * projected[:, 2, 1]
        imag_part = degree * projected[:, 0, 1] - ladder_steps * shifted[:, 1] - orders[:, None] * projected[:, 2, 0]
        return jnp.stack([real_part, imag_part], axis=1) / L
    estimates = lax.map(one_sim, jnp.moveaxis(sim_alm, 1, 0))
    field_sum = lax.optimization_barrier(jnp.sum(estimates, axis=0))
    residual = estimates - field_sum / NSIM
    partner = residual.reshape(NSIM // 2, 2, L, 2, L)[:, ::-1].reshape(residual.shape)
    auto_power = lax.optimization_barrier(jnp.sum(residual * residual, axis=2))
    cross_power = lax.optimization_barrier(jnp.sum(residual * partner, axis=2))
    spectra = jnp.stack([jnp.einsum('m,sml->sl', mode_weight, auto_power, precision=highest), jnp.einsum('m,sml->sl', mode_weight, cross_power, precision=highest)], axis=1)
    spectra = spectra / (2.0 * degree + 1.0)
    return (field_sum, spectra)
```

```python
import functools
import math

import jax
import jax.numpy as jnp
import numpy as np
from jax import lax
from jax.experimental import pallas as pl
from jax.experimental.pallas import tpu as pltpu
from jax.sharding import Mesh
from jax.sharding import PartitionSpec as P

BLK = ("blk_0", "blk_1", "blk_2")
F32 = jnp.float32
BF16 = jnp.bfloat16
STEP = 4


def ladder(degree, orders):
    numerator = (2.0 * degree + 1.0) * (degree * degree - orders * orders)
    denominator = jnp.maximum(2.0 * degree - 1.0, 1.0)
    return jnp.where(degree > orders, jnp.sqrt(jnp.maximum(numerator, 0.0) / denominator), 0.0)


def rounded(x):
    return x.astype(BF16).astype(F32)


def turned(x, shift, axis):
    return pltpu.roll(x, shift % x.shape[axis], axis)


def block_swap(x):
    row = lax.broadcasted_iota(jnp.int32, x.shape, 0) < 4
    lane = lax.broadcasted_iota(jnp.int32, x.shape, 1) < 64
    return jnp.where(row == lane, x, turned(turned(x, 64, 1), 4, 0))


def legendre_sums(x_ref, leg_ref, t_ref, w_ref, lad_ref, cm_ref, trig_ref, out_ref, rows_ref):
    step = pl.program_id(0)
    length = x_ref.shape[2]
    orders = STEP * pl.num_programs(0)
    per_class = 2 * orders
    degree = lax.broadcasted_iota(jnp.int32, (1, length), 1).astype(F32)
    cosecant = trig_ref[0:1, :]
    cotangent = trig_ref[1:2, :]
    sign = jnp.where(lax.broadcasted_iota(jnp.int32, (8, 1), 0) < 4, -1.0, 1.0)

    @pl.when(step == 0)
    def _():
        rows_ref[...] = jnp.zeros_like(rows_ref)

    results = []
    for i in range(STEP):
        values = x_ref[i].astype(F32)
        weighted = w_ref[...] * values
        raised = lad_ref[i] * weighted
        coefs = jnp.concatenate(
            [t_ref[...] * values, weighted, degree * weighted, turned(raised, -1, 1)], axis=0
        ).astype(BF16)
        sums = jnp.dot(coefs, leg_ref[i], preferred_element_type=F32)
        spun = turned(sums[8:16], 4, 0) * (sign * cm_ref[i])
        slopes = cotangent * sums[16:24] - cosecant * sums[24:32]
        results.append((sums[0:8], spun, slopes))
    for q in range(3):
        for c in range(2):
            for par in range(2):
                start = q * 4 * per_class + (2 * c + par) * per_class + 8 * step
                rows_ref[pl.ds(pl.multiple_of(start, 8), 8), :] = jnp.concatenate(
                    [results[par][q][4 * c : 4 * c + 4], results[par + 2][q][4 * c : 4 * c + 4]],
                    axis=0,
                )

    @pl.when(step == pl.num_programs(0) - 1)
    def _():
        for k in range(rows_ref.shape[0] // 128):
            out_ref[:, 128 * k : 128 * k + 128] = rows_ref[128 * k : 128 * k + 128, :].T.astype(
                BF16
            )


def fourier_sums(
    y_ref, ca_ref, sa_ref, cb_ref, sb_ref, mask_ref, tilt_ref,
    mode_ref, tot_ref,
    table, lhs, spread, acc, flow,
    *, scale,
):
    blocks = ca_ref.shape[0]
    orders = cb_ref.shape[0]
    half = orders // 2
    per_class = 2 * orders
    depth = half * blocks
    width = ca_ref.shape[1]

    def turn(h, carry):
        for par in range(2):
            cb = cb_ref[pl.ds(2 * h + par, 1), :]
            sb = sb_ref[pl.ds(2 * h + par, 1), :]
            rows = pl.ds(pl.multiple_of(h * blocks, blocks), blocks)
            for k in range(0, width, 128):
                ca = ca_ref[:, k : k + 128]
                sa = sa_ref[:, k : k + 128]
                cbk = cb[:, k : k + 128]
                sbk = sb[:, k : k + 128]
                table[par, rows, k : k + 128] = (ca * cbk - sa * sbk).astype(BF16)
                table[2 + par, rows, k : k + 128] = (sa * cbk + ca * sbk).astype(BF16)
        return carry

    lax.fori_loop(0, half, turn, 0)

    arrived = []
    for k in range(y_ref.shape[1] // 128):
        spread[k] = y_ref[:, 128 * k : 128 * k + 128].astype(F32)
        cycles = [spread[k, pl.ds(i, blocks, stride=2), :] for i in range(2)]
        arrived.append(jnp.concatenate(cycles, axis=0).T)
    turned_rows = jnp.concatenate(arrived, axis=0)
    lane = lax.broadcasted_iota(jnp.int32, (8, 128), 1)
    for q in range(3):
        for cls in range(4):
            for pair in range(half // 2):
                start = q * 4 * per_class + cls * per_class + 8 * pair
                tile = block_swap(turned_rows[start : start + 8])
                if cls % 2 == 0 and pair == 0:
                    tile = jnp.where(lane == 0, tile, tile * 2.0)
                else:
                    tile = tile * 2.0
                column = cls * depth + 128 * pair
                lhs[8 * q : 8 * q + 8, column : column + 128] = tile.astype(BF16)

    for cls in range(4):
        acc[cls] = jnp.dot(
            lhs[:, cls * depth : (cls + 1) * depth], table[cls], preferred_element_type=F32
        )

    first_cycle = lax.broadcasted_iota(jnp.int32, (8, 128), 0) < 4
    for k in range(0, width, 128):
        ee, eo, oe, oo = (acc[cls, :, k : k + 128] for cls in range(4))
        x, u, y, v = ee + eo, ee - eo, oe + oo, oe - oo
        flows = []
        for quarter, maps in enumerate((x + y, u - v, u + v, x - y)):
            weight = jnp.where(
                first_cycle,
                mask_ref[2 * quarter : 2 * quarter + 1, k : k + 128],
                mask_ref[2 * quarter + 1 : 2 * quarter + 2, k : k + 128],
            )
            product = weight * maps[0:8]
            flows.append(
                rounded(
                    jnp.concatenate([product * maps[16:24], product * maps[8:16]], axis=0)
                )
            )
        f1, f2, f3, f4 = flows
        a, b, c, d = f1 + f4, f2 + f3, f1 - f4, f3 - f2
        for cls, total in enumerate((a + b, a - b, c + d, c - d)):
            high = total.astype(BF16)
            flow[cls, 0:16, k : k + 128] = high
            flow[cls, 16:32, k : k + 128] = (total - high.astype(F32)).astype(BF16)

    for cls in range(4):
        both = lax.dot_general(
            flow[cls], table[cls], (((1,), (1,)), ((), ())), preferred_element_type=F32
        )
        mode = ((both[0:16] + both[16:32]) * scale).astype(BF16)
        columns = slice(cls * depth, (cls + 1) * depth)
        mode_ref[:, columns] = mode
        mode = mode.astype(F32)
        tilted = rounded(tilt_ref[:, 0:1] * mode[0:8])
        parts = []
        for cycle in range(2):
            for rows in (tilted, mode[0:8], mode[8:16]):
                parts.append(jnp.sum(rows[4 * cycle : 4 * cycle + 4], axis=0, keepdims=True))
            parts.append(jnp.zeros_like(parts[0]))
        tot_ref[:, columns] = jnp.concatenate(parts, axis=0)


def pack_modes(mode_ref, mine_ref, other_ref, out_ref, spread):
    blocks = out_ref.shape[0] // 2
    pairs = mode_ref.shape[1] // 128
    total = mine_ref[...].astype(F32) + other_ref[...].astype(F32)
    high = rounded(total)
    mode = mode_ref[...].astype(F32)
    sources = (mode[0:8], mode[8:16], high, total - high)
    rows = jnp.concatenate(
        [
            block_swap(source[:, 128 * pair : 128 * pair + 128])
            for source in sources
            for pair in range(pairs)
        ],
        axis=0,
    )
    for k in range(rows.shape[0] // 128):
        tile = rows[128 * k : 128 * k + 128].T
        spread[k, pl.ds(0, blocks, stride=2), :] = tile[0:blocks]
        spread[k, pl.ds(1, blocks, stride=2), :] = tile[blocks:]
        out_ref[:, 128 * k : 128 * k + 128] = spread[k].astype(BF16)


def estimate_sums(
    order_ref, quarter_ref, z_ref, leg_ref, lad_ref, tilt_ref,
    field_ref, power_ref,
    rows_ref, auto_ref, cross_ref, share_ref,
    *, sim_total,
):
    step = pl.program_id(0)
    length = leg_ref.shape[1]
    per_class = 8 * pl.num_programs(0)
    degree = lax.broadcasted_iota(jnp.int32, (1, length), 1).astype(F32)
    row = lax.broadcasted_iota(jnp.int32, (8, 1), 0)
    sign = jnp.where(row < 4, 1.0, -1.0)
    share = field_ref.shape[2]

    @pl.when(step == 0)
    def _():
        for k in range(z_ref.shape[1] // 128):
            rows_ref[128 * k : 128 * k + 128, :] = (
                z_ref[:, 128 * k : 128 * k + 128].astype(F32).T
            )
        auto_ref[...] = jnp.zeros_like(auto_ref)
        cross_ref[...] = jnp.zeros_like(cross_ref)

    def piece(p, cls):
        start = p * 4 * per_class + cls * per_class + 8 * step
        return rows_ref[pl.ds(pl.multiple_of(start, 8), 8), :]

    pieces = [[piece(p, cls) for cls in range(4)] for p in range(4)]
    for i in range(STEP):
        par, h = i % 2, 4 * (i // 2)
        order = order_ref[STEP * step + i]

        def own(p):
            return jnp.concatenate(
                [pieces[p][par][h : h + 4], pieces[p][2 + par][h : h + 4]], axis=0
            )

        def whole(p, k):
            return jnp.where(
                row < 4, pieces[p][par][h + k : h + k + 1], pieces[p][2 + par][h + k : h + k + 1]
            )

        first, second = own(0), own(1)
        stacked = jnp.concatenate(
            [rounded(tilt_ref[...] * first), first, second]
            + [whole(p, k) for p in (2, 3) for k in range(3)],
            axis=0,
        ).astype(BF16)
        projected = lax.dot_general(
            stacked, leg_ref[i], (((1,), (1,)), ((), ())), preferred_element_type=F32
        )
        steps = lad_ref[i]

        def combine(zero, one, two):
            return (
                degree * zero - steps * turned(one, 1, 1) + (order * sign) * turned(two, 4, 0)
            ) * (1.0 / length)

        estimate = combine(projected[0:8], projected[8:16], projected[16:24])
        field = combine(
            projected[24:32] + projected[48:56],
            projected[32:40] + projected[56:64],
            projected[40:48] + projected[64:72],
        )
        share_ref[...] = field
        mine = share_ref[:, pl.ds(pl.multiple_of(quarter_ref[0] * share, 128), share)]
        field_ref[i] = jnp.concatenate([mine[0:1], mine[4:5]], axis=0)
        residual = estimate - field * (1.0 / sim_total)
        partner = jnp.where(row % 2 == 0, turned(residual, -1, 0), turned(residual, 1, 0))
        doubled = jnp.where(order > 0, 2.0, 1.0) * residual
        auto_ref[...] += doubled * residual
        cross_ref[...] += doubled * partner

    @pl.when(step == pl.num_programs(0) - 1)
    def _():
        power_ref[0:4, :] = auto_ref[0:4, :] + auto_ref[4:8, :]
        power_ref[4:8, :] = cross_ref[0:4, :] + cross_ref[4:8, :]


def exchanged(array, axis, shift=None, flip=None):
    size = lax.axis_size(axis)
    pairs = [(i, i ^ flip if flip else (i + shift) % size) for i in range(size)]
    return lax.ppermute(array, axis, pairs)


def whole_spec(shape):
    return pl.BlockSpec(shape, lambda *_: (0,) * len(shape))


def per_device(sim_alm, t_filter, wiener_filter, colatitude, legendre, pixel_mask):
    orders, sims_here, _, length = sim_alm.shape
    cycles = legendre.shape[2]
    pixels = pixel_mask.shape[1]
    blocks = lax.axis_size(BLK)
    sim_groups = lax.axis_size("sims")
    local_cycles = cycles // blocks
    grid = orders // STEP
    block_id = lax.axis_index(BLK)
    local_orders = (block_id * orders + jnp.arange(orders, dtype=jnp.int32)).astype(F32)
    degree = jnp.arange(length, dtype=F32)
    steps = ladder(degree[None, :], local_orders[:, None])[:, None, :]
    sine = jnp.sin(colatitude)
    cosine = jnp.cos(colatitude)
    cosecant = 1.0 / sine
    trig = jnp.stack([cosecant, cosine / sine])
    turn_scale = (local_orders[:, None] * cosecant[None, :])[:, None, :]
    values = jnp.transpose(sim_alm, (0, 2, 1, 3)).reshape(orders, 2 * sims_here, length)

    wide = -(-3 * 8 * orders // 128) * 128
    coefs = pl.pallas_call(
        legendre_sums,
        grid=(grid,),
        in_specs=[
            pl.BlockSpec((STEP, 8, length), lambda g: (g, 0, 0)),
            pl.BlockSpec((STEP, length, cycles), lambda g: (g, 0, 0)),
            whole_spec((1, length)),
            whole_spec((1, length)),
            pl.BlockSpec((STEP, 1, length), lambda g: (g, 0, 0)),
            pl.BlockSpec((STEP, 1, cycles), lambda g: (g, 0, 0)),
            whole_spec((2, cycles)),
        ],
        out_specs=whole_spec((cycles, wide)),
        out_shape=jax.ShapeDtypeStruct((cycles, wide), BF16),
        scratch_shapes=[pltpu.VMEM((wide, cycles), F32)],
        name="legendre_sums",
    )(values, legendre, t_filter[None], wiener_filter[None], steps, turn_scale, trig)
    arrived = lax.all_to_all(
        coefs.reshape(blocks, local_cycles, wide), BLK, 0, 0, tiled=True
    ).reshape(cycles, wide)

    fold = pixels // 4
    width = -(-(fold + 1) // 128) * 128
    pixel_ids = np.arange(width)
    coarse = 2.0 * np.pi / pixels * (orders * np.arange(blocks)[:, None] * pixel_ids % pixels)
    fine = 2.0 * np.pi / pixels * (np.arange(orders)[:, None] * pixel_ids % pixels)
    weight = pixel_mask.astype(F32)
    inner = jnp.zeros((local_cycles, 1), F32)
    quarters = jnp.stack(
        [
            weight[:, : fold + 1],
            jnp.concatenate([inner, weight[:, fold + 1 : 2 * fold][:, ::-1], inner], axis=1),
            weight[:, 2 * fold : 3 * fold + 1],
            jnp.concatenate([inner, weight[:, 3 * fold + 1 :][:, ::-1], inner], axis=1),
        ]
    ).reshape(4 * local_cycles, fold + 1)
    quarters = jnp.pad(quarters, ((0, 0), (0, width - fold - 1)))
    local_cosine = lax.dynamic_slice_in_dim(cosine, block_id * local_cycles, local_cycles, 0)
    local_tilt = jnp.broadcast_to(jnp.repeat(local_cosine, sims_here)[:, None], (8, 128))
    span = 2 * orders * blocks
    modes, partial_total = pl.pallas_call(
        functools.partial(fourier_sums, scale=2.0 * math.pi / pixels),
        out_shape=[
            jax.ShapeDtypeStruct((16, span), BF16),
            jax.ShapeDtypeStruct((8, span), F32),
        ],
        scratch_shapes=[
            pltpu.VMEM((4, span // 4, width), BF16),
            pltpu.VMEM((24, span), BF16),
            pltpu.VMEM((wide // 128, cycles, 128), F32),
            pltpu.VMEM((4, 24, width), F32),
            pltpu.VMEM((4, 32, width), BF16),
        ],
        name="fourier_sums",
    )(
        arrived,
        np.cos(coarse).astype(np.float32),
        -np.sin(coarse).astype(np.float32),
        np.cos(fine).astype(np.float32),
        -np.sin(fine).astype(np.float32),
        quarters,
        local_tilt,
    )

    chip_total = partial_total + exchanged(partial_total, "sims", flip=1)
    chip_total = chip_total.astype(BF16)
    far_total = exchanged(chip_total, "sims", flip=2)
    packed = pl.pallas_call(
        pack_modes,
        out_shape=jax.ShapeDtypeStruct((cycles, 4 * 8 * orders), BF16),
        scratch_shapes=[pltpu.VMEM((orders // 4, cycles, 128), F32)],
        name="pack_modes",
    )(modes, chip_total, far_total)
    returned = lax.all_to_all(
        packed.reshape(blocks, local_cycles, 32 * orders), BLK, 0, 0, tiled=True
    ).reshape(cycles, 32 * orders)

    share = length // sim_groups
    field_share, power = pl.pallas_call(
        functools.partial(estimate_sums, sim_total=sims_here * sim_groups),
        grid=(grid,),
        in_specs=[
            pl.BlockSpec(memory_space=pltpu.SMEM),
            pl.BlockSpec(memory_space=pltpu.SMEM),
            whole_spec((cycles, 32 * orders)),
            pl.BlockSpec((STEP, length, cycles), lambda g: (g, 0, 0)),
            pl.BlockSpec((STEP, 1, length), lambda g: (g, 0, 0)),
            whole_spec((1, cycles)),
        ],
        out_specs=[
            pl.BlockSpec((STEP, 2, share), lambda g: (g, 0, 0)),
            whole_spec((8, length)),
        ],
        out_shape=[
            jax.ShapeDtypeStruct((orders, 2, share), F32),
            jax.ShapeDtypeStruct((8, length), F32),
        ],
        scratch_shapes=[
            pltpu.VMEM((32 * orders, cycles), F32),
            pltpu.VMEM((8, length), F32),
            pltpu.VMEM((8, length), F32),
            pltpu.VMEM((8, length), F32),
        ],
        name="estimate_sums",
    )(
        local_orders,
        lax.axis_index("sims").astype(jnp.int32)[None],
        returned,
        legendre,
        steps,
        cosine[None],
    )

    for axis in BLK:
        others = [exchanged(power, axis, shift=k) for k in range(1, lax.axis_size(axis))]
        power = power + sum(others)
    spectra = jnp.transpose(power.reshape(2, sims_here, length), (1, 0, 2)) / (2.0 * degree + 1.0)
    return (field_share, spectra)


def solution(mesh):
    torus = Mesh(
        mesh.devices.reshape(mesh.shape["sims"], 4, 4, 4), ("sims", "blk_0", "blk_1", "blk_2")
    )
    return jax.shard_map(
        per_device,
        mesh=torus,
        in_specs=(P(BLK, "sims", None, None), P(), P(), P(), P(BLK, None, None), P(BLK, None)),
        out_specs=(P(BLK, None, "sims"), P("sims", None, None)),
        check_vma=False,
    )
```

```python
import functools
import math

import jax
import jax.numpy as jnp
import numpy as np
from jax import lax
from jax.experimental import pallas as pl
from jax.experimental.pallas import tpu as pltpu
from jax.sharding import Mesh
from jax.sharding import PartitionSpec as P

BLK = ("blk_0", "blk_1", "blk_2")
F32 = jnp.float32
BF16 = jnp.bfloat16
ROOM = pltpu.CompilerParams(vmem_limit_bytes=52 << 20)
STEP = 4


def ladder(degree, orders):
    numerator = (2.0 * degree + 1.0) * (degree * degree - orders * orders)
    denominator = jnp.maximum(2.0 * degree - 1.0, 1.0)
    return jnp.where(degree > orders, jnp.sqrt(jnp.maximum(numerator, 0.0) / denominator), 0.0)


def rounded(x):
    return x.astype(BF16).astype(F32)


def turned(x, shift, axis):
    return pltpu.roll(x, shift % x.shape[axis], axis)


def block_swap(x):
    row = lax.broadcasted_iota(jnp.int32, x.shape, 0) < 4
    lane = lax.broadcasted_iota(jnp.int32, x.shape, 1) < 64
    return jnp.where(row == lane, x, turned(turned(x, 64, 1), 4, 0))


def fetch(source, target, sems, n):
    rows = pl.ds(pl.multiple_of(n * STEP, STEP), STEP)
    return pltpu.make_async_copy(source.at[rows], target.at[rows], sems.at[n])


def copies(sources, targets, sems):
    return [
        pltpu.make_async_copy(source, target, sems.at[n])
        for n, (source, target) in enumerate(zip(sources, targets))
    ]


def first_order(orders):
    return lax.axis_index(BLK) * orders


def ladder_rows(orders, length):
    degree = lax.broadcasted_iota(jnp.int32, (orders, length), 1).astype(F32)
    order = (first_order(orders) + lax.broadcasted_iota(jnp.int32, (orders, length), 0)).astype(F32)
    return ladder(degree, order)


def legendre_sums(
    x_hbm, leg_hbm, t_hbm, w_hbm, angle_hbm,
    out_ref,
    x_ref, leg_ref, t_ref, w_ref, angle_ref, lad_ref, sums_ref, rows_ref, small_sems, leg_sems,
):
    orders, length = leg_ref.shape[:2]
    small = copies(
        (angle_hbm, t_hbm, w_hbm, x_hbm), (angle_ref, t_ref, w_ref, x_ref), small_sems
    )
    for copy in small + [fetch(leg_hbm, leg_ref, leg_sems, 0)]:
        copy.start()

    lad_ref[...] = ladder_rows(orders, length)
    rows_ref[...] = jnp.zeros_like(rows_ref)
    degree = lax.broadcasted_iota(jnp.int32, (1, length), 1).astype(F32)
    first_half = lax.broadcasted_iota(jnp.int32, (8, 1), 0) < 4
    first = first_order(orders)
    per_class = 2 * orders
    for copy in small:
        copy.wait()
    fetch(leg_hbm, leg_ref, leg_sems, 1).start()
    angle = angle_ref[...][None, :]
    cosecant = 1.0 / jnp.sin(angle)
    cotangent = jnp.cos(angle) / jnp.sin(angle)
    t_row = t_ref[...][None, :]
    w_row = w_ref[...][None, :]

    def some(step, carry):
        start = pl.multiple_of(step * STEP, STEP)
        fetch(leg_hbm, leg_ref, leg_sems, step).wait()

        @pl.when(step + 2 < orders // STEP)
        def _():
            fetch(leg_hbm, leg_ref, leg_sems, step + 2).start()

        for i in range(STEP):
            values = x_ref[start + i].astype(F32).reshape(8, length)
            weighted = w_row * values
            raised = lad_ref[pl.ds(start + i, 1), :] * weighted
            coefs = jnp.concatenate(
                [t_row * values, weighted, degree * weighted, turned(raised, -1, 1)], axis=0
            ).astype(BF16)
            sums_ref[i] = jnp.dot(coefs, leg_ref[start + i], preferred_element_type=F32)
        for par in range(2):

            def pair(k, c):
                return jnp.concatenate(
                    [sums_ref[i, pl.ds(8 * k + c, 4, stride=2), :] for i in (par, par + 2)], axis=0
                )

            order = jnp.where(first_half, first + start + par, first + start + par + 2)
            spin = order.astype(F32) * cosecant
            for c in range(2):
                spun = pair(1, 1 - c) * spin
                slopes = cotangent * pair(2, c) - cosecant * pair(3, c)
                for q, rows in enumerate((pair(0, c), spun if c else -spun, slopes)):
                    place = q * 4 * per_class + (2 * c + par) * per_class
                    rows_ref[pl.ds(pl.multiple_of(place + 8 * step, 8), 8), :] = rows
        return carry

    lax.fori_loop(0, orders // STEP, some, 0)
    for k in range(rows_ref.shape[0] // 128):
        columns = slice(128 * k, 128 * k + 128)
        out_ref[:, :, columns] = rows_ref[columns, :].T.reshape(-1, 2, 128).astype(BF16)


def table_rows(turns, blocks, order, cosines, sines, rows):
    orders = turns.shape[0] // 2 - blocks
    cb_row = turns[pl.ds(2 * blocks + order, 1), :]
    sb_row = turns[pl.ds(2 * blocks + orders + order, 1), :]
    for k in range(0, turns.shape[1], 128):
        columns = slice(k, k + 128)
        ca = turns[:blocks, columns]
        sa = turns[blocks : 2 * blocks, columns]
        cb = cb_row[:, columns]
        sb = sb_row[:, columns]
        cosines[rows, columns] = (ca * cb - sa * sb).astype(BF16)
        sines[rows, columns] = (sa * cb + ca * sb).astype(BF16)


def make_table(
    turns, pixel_ref,
    table_hbm, lad_ref, quarter_ref,
    table, sems,
):
    width = turns.shape[1]
    orders = lad_ref.shape[0]
    blocks = turns.shape[0] // 2 - orders

    def stores(h):
        rows = pl.ds(pl.multiple_of(h * blocks, blocks), blocks)
        return [
            pltpu.make_async_copy(table.at[c, rows], table_hbm.at[c, rows], sems.at[h, c])
            for c in range(2)
        ]

    def turn(h, carry):
        rows = pl.ds(pl.multiple_of(h * blocks, blocks), blocks)
        table_rows(turns, blocks, 2 * h, table.at[0], table.at[1], rows)
        for copy in stores(h):
            copy.start()
        return carry

    lax.fori_loop(0, orders // 2, turn, 0)

    lad_ref[...] = ladder_rows(orders, lad_ref.shape[1])

    fold = pixel_ref.shape[1] // 4
    weight = pixel_ref[...].astype(F32)
    cycles = weight.shape[0]
    end = jnp.zeros((cycles, width - fold), F32)
    lane = lax.broadcasted_iota(jnp.int32, (cycles, width), 1)
    row = lax.broadcasted_iota(jnp.int32, (128, 128), 0)
    column = lax.broadcasted_iota(jnp.int32, (128, 128), 1)
    flip = jnp.where(row + column == 127, 1.0, 0.0).astype(BF16)
    for n in range(2):
        near = weight[:, 2 * n * fold : (2 * n + 1) * fold]
        far = weight[:, (2 * n + 1) * fold : (2 * n + 2) * fold]
        flipped = jnp.concatenate(
            [
                jnp.dot(far[:, k : k + 128].astype(BF16), flip, preferred_element_type=F32)
                for k in range(fold - 128, -1, -128)
            ],
            axis=1,
        )
        first = jnp.concatenate([near, end], axis=1)
        second = jnp.concatenate([turned(flipped, 1, 1), end], axis=1)
        quarter_ref[4 * n : 4 * n + 2, :] = jnp.where(lane == fold, turned_edge(far, lane), first)
        quarter_ref[4 * n + 2 : 4 * n + 4, :] = jnp.where(lane == 0, 0.0, second)

    def finish(h, carry):
        for copy in stores(h):
            copy.wait()
        return carry

    lax.fori_loop(0, orders // 2, finish, 0)


def turned_edge(far, lane):
    return jnp.broadcast_to(far[:, 0:1], lane.shape)


def fourier_sums(
    y_hbm, table_hbm, mask_hbm, angle_hbm, turns_hbm,
    own_ref, tot_ref,
    y_ref, table, mask_ref, angle_ref, turns,
    lhs, spread, acc, flow, rows_ref, table_sems, small_sems,
    *, scale, orders,
):
    blocks, cycles = y_ref.shape[:2]
    half = orders // 2
    per_class = 2 * orders
    depth = half * blocks
    width = table.shape[2]
    small = copies(
        (turns_hbm, y_hbm, mask_hbm, angle_hbm), (turns, y_ref, mask_ref, angle_ref), small_sems
    )
    loads = [
        pltpu.make_async_copy(table_hbm.at[c], table.at[2 * c], table_sems.at[c]) for c in range(2)
    ]
    for copy in small:
        copy.start()
    for copy in small[1:]:
        copy.wait()
    for copy in loads:
        copy.start()

    arrived = []
    for k in range(y_ref.shape[2] // 128):
        spread[k] = y_ref[:, :, 128 * k : 128 * k + 128].astype(F32).reshape(-1, 128)
        parts = [spread[k, pl.ds(i, blocks, stride=2), :] for i in range(2)]
        arrived.append(jnp.concatenate(parts, axis=0).T)
    turned_rows = jnp.concatenate(arrived, axis=0)
    lane = lax.broadcasted_iota(jnp.int32, (8, 128), 1)
    for cls in range(4):
        for pair in range(half // 2):
            tiles = []
            for q in range(3):
                start = q * 4 * per_class + cls * per_class + 8 * pair
                tile = block_swap(turned_rows[start : start + 8])
                if cls % 2 == 0 and pair == 0:
                    tiles.append(jnp.where(lane == 0, tile, tile * 2.0))
                else:
                    tiles.append(tile * 2.0)
            column = cls * depth + 128 * pair
            lhs[:, column : column + 128] = jnp.concatenate(tiles, axis=0).astype(BF16)

    small[0].wait()

    def turn(h, carry):
        rows = pl.ds(pl.multiple_of(h * blocks, blocks), blocks)
        table_rows(turns, blocks, 2 * h + 1, table.at[1], table.at[3], rows)
        return carry

    lax.fori_loop(0, half, turn, 0)
    for cls in (1, 3, 0, 2):
        if cls % 2 == 0:
            loads[cls // 2].wait()
        acc[cls] = jnp.dot(
            lhs[:, cls * depth : (cls + 1) * depth], table[cls], preferred_element_type=F32
        )

    first_cycle = lax.broadcasted_iota(jnp.int32, (8, 128), 0) < 4
    for k in range(0, width, 128):
        ee, eo, oe, oo = (acc[cls, :, k : k + 128] for cls in range(4))
        x, u, y, v = ee + eo, ee - eo, oe + oo, oe - oo
        flows = []
        for quarter, maps in enumerate((x + y, u - v, u + v, x - y)):
            weight = jnp.where(
                first_cycle,
                mask_ref[2 * quarter : 2 * quarter + 1, k : k + 128],
                mask_ref[2 * quarter + 1 : 2 * quarter + 2, k : k + 128],
            )
            product = weight * maps[0:8]
            flows.append(
                rounded(
                    jnp.concatenate([product * maps[16:24], product * maps[8:16]], axis=0)
                )
            )
        f1, f2, f3, f4 = flows
        a, b, c, d = f1 + f4, f2 + f3, f1 - f4, f3 - f2
        for cls, total in enumerate((a + b, a - b, c + d, c - d)):
            high = total.astype(BF16)
            flow[cls, :, k : k + 128] = jnp.concatenate(
                [high, (total - high.astype(F32)).astype(BF16)], axis=0
            )

    tilts = jnp.cos(angle_ref[...][None, :])
    place = lax.broadcasted_iota(jnp.int32, tilts.shape, 1) - lax.axis_index(BLK) * cycles
    tilt = [
        jnp.sum(jnp.where(place == i, tilts, 0.0), axis=1, keepdims=True) for i in range(cycles)
    ]
    tilt = jnp.where(lax.broadcasted_iota(jnp.int32, (8, 1), 0) < 4, tilt[0], tilt[1])
    for cls in range(4):
        both = lax.dot_general(
            flow[cls], table[cls], (((1,), (1,)), ((), ())), preferred_element_type=F32
        )
        mode = rounded((both[0:16] + both[16:32]) * scale)
        tilted = rounded(tilt * mode[0:8])
        parts = []
        for cycle in range(2):
            for rows in (tilted, mode[0:8], mode[8:16]):
                parts.append(jnp.sum(rows[4 * cycle : 4 * cycle + 4], axis=0, keepdims=True))
            parts.append(jnp.zeros_like(parts[0]))
        tot_ref[:, cls * depth : (cls + 1) * depth] = jnp.concatenate(parts, axis=0).astype(BF16)
        for p in range(2):
            for pair in range(half // 2):
                start = p * 4 * per_class + cls * per_class + 8 * pair
                rows_ref[start : start + 8, :] = block_swap(
                    mode[8 * p : 8 * p + 8, 128 * pair : 128 * pair + 128]
                )
    pack(rows_ref, own_ref, spread, 0)


def pack(rows_ref, out_ref, spread, first_column):
    blocks = out_ref.shape[0]
    for k in range(rows_ref.shape[0] // 128):
        tile = rows_ref[128 * k : 128 * k + 128, :].T
        spread[k, pl.ds(0, blocks, stride=2), :] = tile[0:blocks]
        spread[k, pl.ds(1, blocks, stride=2), :] = tile[blocks:]
        column = first_column + 128 * k
        out_ref[:, :, column : column + 128] = spread[k].reshape(blocks, 2, 128).astype(BF16)


def pack_totals(own_ref, mine_ref, near_ref, far_ref, near_far_ref, out_ref, spread, rows_ref):
    pairs = mine_ref.shape[1] // 128
    own_width = own_ref.shape[2]
    out_ref[:, :, :own_width] = own_ref[...]
    parts = (mine_ref, near_ref, far_ref, near_far_ref)
    total = sum(part[...].astype(F32) for part in parts)
    high = rounded(total)
    low = total - high
    for n, source in enumerate((high, low)):
        for pair in range(pairs):
            start = 8 * (n * pairs + pair)
            rows_ref[start : start + 8, :] = block_swap(source[:, 128 * pair : 128 * pair + 128])
    pack(rows_ref, out_ref, spread, own_width)


def estimate_sums(
    z_hbm, leg_hbm, lad_hbm, angle_hbm,
    field_ref, power_ref,
    z_ref, leg_ref, lad_ref, angle_ref,
    rows_ref, auto_ref, cross_ref, share_ref, leg_sems, small_sems,
    *, sim_total,
):
    orders, length = leg_ref.shape[:2]
    small = copies((z_hbm, angle_hbm, lad_hbm), (z_ref, angle_ref, lad_ref), small_sems)
    for copy in small + [fetch(leg_hbm, leg_ref, leg_sems, 0)]:
        copy.start()
    per_class = 2 * orders
    degree = lax.broadcasted_iota(jnp.int32, (1, length), 1).astype(F32)
    row = lax.broadcasted_iota(jnp.int32, (8, 1), 0)
    sign = jnp.where(row < 4, 1.0, -1.0)
    share = field_ref.shape[2]
    here = pl.ds(pl.multiple_of(lax.axis_index("sims") * share, 128), share)
    first = first_order(orders)
    for copy in small:
        copy.wait()
    fetch(leg_hbm, leg_ref, leg_sems, 1).start()
    tilt = jnp.cos(angle_ref[...][None, :])
    for k in range(z_ref.shape[2] // 128):
        columns = slice(128 * k, 128 * k + 128)
        rows_ref[columns, :] = z_ref[:, :, columns].astype(F32).reshape(-1, 128).T
    auto_ref[...] = jnp.zeros_like(auto_ref)
    cross_ref[...] = jnp.zeros_like(cross_ref)

    def some(step, carry):
        start = pl.multiple_of(step * STEP, STEP)
        fetch(leg_hbm, leg_ref, leg_sems, step).wait()

        @pl.when(step + 2 < orders // STEP)
        def _():
            fetch(leg_hbm, leg_ref, leg_sems, step + 2).start()


        def piece(p, cls):
            place = p * 4 * per_class + cls * per_class + 8 * step
            return rows_ref[pl.ds(pl.multiple_of(place, 8), 8), :]

        pieces = [[piece(p, cls) for cls in range(4)] for p in range(4)]
        auto = auto_ref[...]
        cross = cross_ref[...]
        for i in range(STEP):
            par, h = i % 2, 4 * (i // 2)
            order = (first + start + i).astype(F32)

            def own(p):
                return jnp.concatenate(
                    [pieces[p][par][h : h + 4], pieces[p][2 + par][h : h + 4]], axis=0
                )

            def whole(p, k):
                return jnp.where(
                    row < 4,
                    pieces[p][par][h + k : h + k + 1],
                    pieces[p][2 + par][h + k : h + k + 1],
                )

            first_mode, second_mode = own(0), own(1)
            stacked = jnp.concatenate(
                [rounded(tilt * first_mode), first_mode, second_mode]
                + [whole(p, k) for p in (2, 3) for k in range(3)],
                axis=0,
            ).astype(BF16)
            projected = lax.dot_general(
                stacked, leg_ref[start + i], (((1,), (1,)), ((), ())), preferred_element_type=F32
            )
            steps = lad_ref[pl.ds(start + i, 1), :]

            def combine(zero, one, two):
                return (
                    degree * zero - steps * turned(one, 1, 1) + (order * sign) * turned(two, 4, 0)
                ) * (1.0 / length)

            estimate = combine(projected[0:8], projected[8:16], projected[16:24])
            field = combine(
                projected[24:32] + projected[48:56],
                projected[32:40] + projected[56:64],
                projected[40:48] + projected[64:72],
            )
            share_ref[i] = field
            mine = share_ref[i, :, here]
            field_ref[start + i] = jnp.concatenate([mine[0:1], mine[4:5]], axis=0)
            residual = estimate - field * (1.0 / sim_total)
            partner = jnp.where(row % 2 == 0, turned(residual, -1, 0), turned(residual, 1, 0))
            doubled = jnp.where(order > 0, 2.0, 1.0) * residual
            auto = auto + doubled * residual
            cross = cross + doubled * partner
        auto_ref[...] = auto
        cross_ref[...] = cross
        return carry

    lax.fori_loop(0, orders // STEP, some, 0)
    auto = auto_ref[0:4, :] + auto_ref[4:8, :]
    cross = cross_ref[0:4, :] + cross_ref[4:8, :]
    for s in range(4):
        power_ref[s] = jnp.concatenate([auto[s : s + 1], cross[s : s + 1]], axis=0)


def exchanged(array, axis, shift=None, flip=None):
    size = lax.axis_size(axis)
    pairs = [(i, i ^ flip if flip else (i + shift) % size) for i in range(size)]
    return lax.ppermute(array, axis, pairs)


def per_device(sim_alm, t_filter, wiener_filter, colatitude, legendre, pixel_mask):
    orders, sims_here, _, length = sim_alm.shape
    cycles = legendre.shape[2]
    pixels = pixel_mask.shape[1]
    blocks = lax.axis_size(BLK)
    sim_groups = lax.axis_size("sims")
    local_cycles = cycles // blocks
    grid = orders // STEP
    degree = jnp.arange(length, dtype=F32)
    outside = pl.BlockSpec(memory_space=pl.ANY)
    inside = pl.BlockSpec(memory_space=pltpu.VMEM)

    wide = -(-3 * 8 * orders // 128) * 128
    coefs = pl.pallas_call(
        legendre_sums,
        in_specs=[outside] * 5,
        out_specs=inside,
        out_shape=jax.ShapeDtypeStruct((blocks, local_cycles, wide), BF16),
        scratch_shapes=[
            pltpu.VMEM(sim_alm.shape, BF16),
            pltpu.VMEM(legendre.shape, BF16),
            pltpu.VMEM((length,), F32),
            pltpu.VMEM((length,), F32),
            pltpu.VMEM((cycles,), F32),
            pltpu.VMEM((orders, length), F32),
            pltpu.VMEM((STEP, 32, cycles), F32),
            pltpu.VMEM((wide, cycles), F32),
            pltpu.SemaphoreType.DMA((4,)),
            pltpu.SemaphoreType.DMA((grid,)),
        ],
        name="legendre_sums",
    )(sim_alm, legendre, t_filter, wiener_filter, colatitude)
    arrived = lax.all_to_all(coefs, BLK, 0, 0, tiled=True)

    fold = pixels // 4
    width = -(-(fold + 1) // 128) * 128
    span = 2 * orders * blocks
    pixel_ids = np.arange(width)
    coarse = 2.0 * np.pi / pixels * (orders * np.arange(blocks)[:, None] * pixel_ids % pixels)
    fine = 2.0 * np.pi / pixels * (np.arange(orders)[:, None] * pixel_ids % pixels)
    turns = np.concatenate(
        [np.cos(coarse), -np.sin(coarse), np.cos(fine), -np.sin(fine)]
    ).astype(np.float32)
    half_table = (2, span // 4, width)
    table, steps, quarters = pl.pallas_call(
        make_table,
        in_specs=[inside] * 2,
        out_specs=[outside, inside, inside],
        out_shape=[
            jax.ShapeDtypeStruct(half_table, BF16),
            jax.ShapeDtypeStruct((orders, length), F32),
            jax.ShapeDtypeStruct((4 * local_cycles, width), F32),
        ],
        scratch_shapes=[
            pltpu.VMEM(half_table, BF16),
            pltpu.SemaphoreType.DMA((orders // 2, 2)),
        ],
        cost_estimate=pl.CostEstimate(
            flops=3 * span * width, bytes_accessed=span * width, transcendentals=0
        ),
        compiler_params=ROOM,
        name="make_table",
    )(
        turns,
        pixel_mask,
    )

    own, partial_total = pl.pallas_call(
        functools.partial(fourier_sums, scale=2.0 * math.pi / pixels, orders=orders),
        in_specs=[outside] * 5,
        out_shape=[
            jax.ShapeDtypeStruct((blocks, local_cycles, 16 * orders), BF16),
            jax.ShapeDtypeStruct((8, span), BF16),
        ],
        scratch_shapes=[
            pltpu.VMEM(coefs.shape, BF16),
            pltpu.VMEM((4, span // 4, width), BF16),
            pltpu.VMEM((4 * local_cycles, width), F32),
            pltpu.VMEM((cycles,), F32),
            pltpu.VMEM(turns.shape, F32),
            pltpu.VMEM((24, span), BF16),
            pltpu.VMEM((wide // 128, cycles, 128), F32),
            pltpu.VMEM((4, 24, width), F32),
            pltpu.VMEM((4, 32, width), BF16),
            pltpu.VMEM((16 * orders, cycles), F32),
            pltpu.SemaphoreType.DMA((2,)),
            pltpu.SemaphoreType.DMA((4,)),
        ],
        compiler_params=ROOM,
        name="fourier_sums",
    )(arrived, table, quarters, colatitude, turns)

    far = exchanged(partial_total, "sims", flip=2)
    near = exchanged(partial_total, "sims", flip=1)
    near_far = exchanged(far, "sims", flip=1)
    packed = pl.pallas_call(
        pack_totals,
        out_shape=jax.ShapeDtypeStruct((blocks, local_cycles, 32 * orders), BF16),
        scratch_shapes=[
            pltpu.VMEM((orders // 8, cycles, 128), F32),
            pltpu.VMEM((16 * orders, cycles), F32),
        ],
        compiler_params=ROOM,
        name="pack_totals",
    )(own, partial_total, near, far, near_far)
    returned = lax.all_to_all(packed, BLK, 0, 0, tiled=True)

    field_share, power = pl.pallas_call(
        functools.partial(estimate_sums, sim_total=sims_here * sim_groups),
        in_specs=[outside] * 4,
        out_shape=[
            jax.ShapeDtypeStruct((orders, 2, length // sim_groups), F32),
            jax.ShapeDtypeStruct((sims_here, 2, length), F32),
        ],
        scratch_shapes=[
            pltpu.VMEM(returned.shape, BF16),
            pltpu.VMEM(legendre.shape, BF16),
            pltpu.VMEM((orders, length), F32),
            pltpu.VMEM((cycles,), F32),
            pltpu.VMEM((32 * orders, cycles), F32),
            pltpu.VMEM((8, length), F32),
            pltpu.VMEM((8, length), F32),
            pltpu.VMEM((STEP, 8, length), F32),
            pltpu.SemaphoreType.DMA((grid,)),
            pltpu.SemaphoreType.DMA((3,)),
        ],
        compiler_params=ROOM,
        name="estimate_sums",
    )(returned, legendre, steps, colatitude)

    for axis in BLK:
        others = [exchanged(power, axis, shift=k) for k in range(1, lax.axis_size(axis))]
        power = power + sum(others)
    return (field_share, power / (2.0 * degree + 1.0))


def solution(mesh):
    torus = Mesh(
        mesh.devices.reshape(mesh.shape["sims"], 4, 4, 4), ("sims", "blk_0", "blk_1", "blk_2")
    )
    return jax.shard_map(
        per_device,
        mesh=torus,
        in_specs=(P(BLK, "sims", None, None), P(), P(), P(), P(BLK, None, None), P(BLK, None)),
        out_specs=(P(BLK, None, "sims"), P("sims", None, None)),
        check_vma=False,
    )
```

```python
import functools
import math

import jax
import jax.numpy as jnp
import numpy as np
from jax import lax
from jax.experimental import pallas as pl
from jax.experimental.pallas import tpu as pltpu
from jax.sharding import Mesh
from jax.sharding import PartitionSpec as P

BLK = ("blk_0", "blk_1", "blk_2")
F32 = jnp.float32
BF16 = jnp.bfloat16
ROOM = pltpu.CompilerParams(vmem_limit_bytes=52 << 20)
AHEAD = 5
STEP = 4


def ladder(degree, orders):
    numerator = (2.0 * degree + 1.0) * (degree * degree - orders * orders)
    denominator = jnp.maximum(2.0 * degree - 1.0, 1.0)
    return jnp.where(degree > orders, jnp.sqrt(jnp.maximum(numerator, 0.0) / denominator), 0.0)


def rounded(x):
    return x.astype(BF16).astype(F32)


def turned(x, shift, axis):
    return pltpu.roll(x, shift % x.shape[axis], axis)


def block_swap(x):
    row = lax.broadcasted_iota(jnp.int32, x.shape, 0) < 4
    lane = lax.broadcasted_iota(jnp.int32, x.shape, 1) < 64
    return jnp.where(row == lane, x, turned(turned(x, 64, 1), 4, 0))


def fetch(source, target, sems, n):
    rows = pl.ds(pl.multiple_of(n * STEP, STEP), STEP)
    return pltpu.make_async_copy(source.at[rows], target.at[rows], sems.at[n])


def copies(sources, targets, sems):
    return [
        pltpu.make_async_copy(source, target, sems.at[n])
        for n, (source, target) in enumerate(zip(sources, targets))
    ]


def first_order(orders):
    return lax.axis_index(BLK) * orders


def ladder_rows(orders, length):
    degree = lax.broadcasted_iota(jnp.int32, (orders, length), 1).astype(F32)
    order = (first_order(orders) + lax.broadcasted_iota(jnp.int32, (orders, length), 0)).astype(F32)
    return ladder(degree, order)


def legendre_sums(
    x_hbm, leg_hbm, t_hbm, w_hbm, angle_hbm,
    out_ref,
    x_ref, leg_ref, t_ref, w_ref, angle_ref, lad_ref, sums_ref, rows_ref, small_sems, leg_sems,
):
    orders, length = leg_ref.shape[:2]
    small = copies(
        (angle_hbm, t_hbm, w_hbm, x_hbm), (angle_ref, t_ref, w_ref, x_ref), small_sems
    )
    for copy in small + [fetch(leg_hbm, leg_ref, leg_sems, 0)]:
        copy.start()

    lad_ref[...] = ladder_rows(orders, length)
    rows_ref[...] = jnp.zeros_like(rows_ref)
    degree = lax.broadcasted_iota(jnp.int32, (1, length), 1).astype(F32)
    first_half = lax.broadcasted_iota(jnp.int32, (8, 1), 0) < 4
    first = first_order(orders)
    per_class = 2 * orders
    for copy in small:
        copy.wait()
    for n in range(1, AHEAD):
        fetch(leg_hbm, leg_ref, leg_sems, n).start()
    angle = angle_ref[...][None, :]
    cosecant = 1.0 / jnp.sin(angle)
    cotangent = jnp.cos(angle) / jnp.sin(angle)
    t_row = t_ref[...][None, :]
    w_row = w_ref[...][None, :]

    def some(step, carry):
        start = pl.multiple_of(step * STEP, STEP)
        fetch(leg_hbm, leg_ref, leg_sems, step).wait()

        @pl.when(step + AHEAD < orders // STEP)
        def _():
            fetch(leg_hbm, leg_ref, leg_sems, step + AHEAD).start()

        for i in range(STEP):
            values = x_ref[start + i].astype(F32).reshape(8, length)
            weighted = w_row * values
            raised = lad_ref[pl.ds(start + i, 1), :] * weighted
            coefs = jnp.concatenate(
                [t_row * values, weighted, degree * weighted, turned(raised, -1, 1)], axis=0
            ).astype(BF16)
            sums_ref[i] = jnp.dot(coefs, leg_ref[start + i], preferred_element_type=F32)
        for par in range(2):

            def pair(k, c):
                return jnp.concatenate(
                    [sums_ref[i, pl.ds(8 * k + c, 4, stride=2), :] for i in (par, par + 2)], axis=0
                )

            order = jnp.where(first_half, first + start + par, first + start + par + 2)
            spin = order.astype(F32) * cosecant
            for c in range(2):
                spun = pair(1, 1 - c) * spin
                slopes = cotangent * pair(2, c) - cosecant * pair(3, c)
                for q, rows in enumerate((pair(0, c), spun if c else -spun, slopes)):
                    place = q * 4 * per_class + (2 * c + par) * per_class
                    rows_ref[pl.ds(pl.multiple_of(place + 8 * step, 8), 8), :] = rows
        return carry

    lax.fori_loop(0, orders // STEP, some, 0)
    for k in range(rows_ref.shape[0] // 128):
        columns = slice(128 * k, 128 * k + 128)
        out_ref[:, :, columns] = rows_ref[columns, :].T.reshape(-1, 2, 128).astype(BF16)


def table_rows(turns, blocks, order, cosines, sines, rows):
    orders = turns.shape[0] // 2 - blocks
    cb_row = turns[pl.ds(2 * blocks + order, 1), :]
    sb_row = turns[pl.ds(2 * blocks + orders + order, 1), :]
    for k in range(0, turns.shape[1], 128):
        columns = slice(k, k + 128)
        ca = turns[:blocks, columns]
        sa = turns[blocks : 2 * blocks, columns]
        cb = cb_row[:, columns]
        sb = sb_row[:, columns]
        cosines[rows, columns] = (ca * cb - sa * sb).astype(BF16)
        sines[rows, columns] = (sa * cb + ca * sb).astype(BF16)


def make_table(
    turns, pixel_ref, leg_hbm,
    table_hbm, lad_ref, quarter_ref, lead_ref,
    table, sems, lead_sem,
):
    lead = pltpu.make_async_copy(leg_hbm.at[pl.ds(0, STEP)], lead_ref, lead_sem)
    lead.start()
    width = turns.shape[1]
    orders = lad_ref.shape[0]
    blocks = turns.shape[0] // 2 - orders

    def stores(h):
        rows = pl.ds(pl.multiple_of(h * blocks, blocks), blocks)
        return [
            pltpu.make_async_copy(table.at[c, rows], table_hbm.at[c, rows], sems.at[h, c])
            for c in range(2)
        ]

    def turn(h, carry):
        rows = pl.ds(pl.multiple_of(h * blocks, blocks), blocks)
        table_rows(turns, blocks, 2 * h, table.at[0], table.at[1], rows)
        for copy in stores(h):
            copy.start()
        return carry

    lax.fori_loop(0, orders // 2, turn, 0)

    lad_ref[...] = ladder_rows(orders, lad_ref.shape[1])

    fold = pixel_ref.shape[1] // 4
    weight = pixel_ref[...].astype(F32)
    cycles = weight.shape[0]
    end = jnp.zeros((cycles, width - fold), F32)
    lane = lax.broadcasted_iota(jnp.int32, (cycles, width), 1)
    row = lax.broadcasted_iota(jnp.int32, (128, 128), 0)
    column = lax.broadcasted_iota(jnp.int32, (128, 128), 1)
    flip = jnp.where(row + column == 127, 1.0, 0.0).astype(BF16)
    for n in range(2):
        near = weight[:, 2 * n * fold : (2 * n + 1) * fold]
        far = weight[:, (2 * n + 1) * fold : (2 * n + 2) * fold]
        flipped = jnp.concatenate(
            [
                jnp.dot(far[:, k : k + 128].astype(BF16), flip, preferred_element_type=F32)
                for k in range(fold - 128, -1, -128)
            ],
            axis=1,
        )
        first = jnp.concatenate([near, end], axis=1)
        second = jnp.concatenate([turned(flipped, 1, 1), end], axis=1)
        quarter_ref[4 * n : 4 * n + 2, :] = jnp.where(lane == fold, turned_edge(far, lane), first)
        quarter_ref[4 * n + 2 : 4 * n + 4, :] = jnp.where(lane == 0, 0.0, second)

    def finish(h, carry):
        for copy in stores(h):
            copy.wait()
        return carry

    lax.fori_loop(0, orders // 2, finish, 0)
    lead.wait()


def turned_edge(far, lane):
    return jnp.broadcast_to(far[:, 0:1], lane.shape)


def fourier_sums(
    y_ref, table_hbm, mask_ref, angle_ref, turns,
    own_ref, tot_ref,
    table, lhs, spread, acc, flow, rows_ref, table_sems,
    *, scale, orders,
):
    blocks, cycles = y_ref.shape[:2]
    half = orders // 2
    per_class = 2 * orders
    depth = half * blocks
    width = table.shape[2]
    loads = [
        pltpu.make_async_copy(table_hbm.at[c], table.at[2 * c], table_sems.at[c]) for c in range(2)
    ]
    for copy in loads:
        copy.start()

    arrived = []
    for k in range(y_ref.shape[2] // 128):
        spread[k] = y_ref[:, :, 128 * k : 128 * k + 128].astype(F32).reshape(-1, 128)
        parts = [spread[k, pl.ds(i, blocks, stride=2), :] for i in range(2)]
        arrived.append(jnp.concatenate(parts, axis=0).T)
    turned_rows = jnp.concatenate(arrived, axis=0)
    lane = lax.broadcasted_iota(jnp.int32, (8, 128), 1)
    for cls in range(4):
        for pair in range(half // 2):
            tiles = []
            for q in range(3):
                start = q * 4 * per_class + cls * per_class + 8 * pair
                tile = block_swap(turned_rows[start : start + 8])
                if cls % 2 == 0 and pair == 0:
                    tiles.append(jnp.where(lane == 0, tile, tile * 2.0))
                else:
                    tiles.append(tile * 2.0)
            column = cls * depth + 128 * pair
            lhs[:, column : column + 128] = jnp.concatenate(tiles, axis=0).astype(BF16)

    def turn(h, carry):
        rows = pl.ds(pl.multiple_of(h * blocks, blocks), blocks)
        table_rows(turns, blocks, 2 * h + 1, table.at[1], table.at[3], rows)
        return carry

    lax.fori_loop(0, half, turn, 0)
    for cls in (1, 3, 0, 2):
        if cls % 2 == 0:
            loads[cls // 2].wait()
        acc[cls] = jnp.dot(
            lhs[:, cls * depth : (cls + 1) * depth], table[cls], preferred_element_type=F32
        )

    first_cycle = lax.broadcasted_iota(jnp.int32, (8, 128), 0) < 4
    for k in range(0, width, 128):
        ee, eo, oe, oo = (acc[cls, :, k : k + 128] for cls in range(4))
        x, u, y, v = ee + eo, ee - eo, oe + oo, oe - oo
        flows = []
        for quarter, maps in enumerate((x + y, u - v, u + v, x - y)):
            weight = jnp.where(
                first_cycle,
                mask_ref[2 * quarter : 2 * quarter + 1, k : k + 128],
                mask_ref[2 * quarter + 1 : 2 * quarter + 2, k : k + 128],
            )
            product = weight * maps[0:8]
            flows.append(
                rounded(
                    jnp.concatenate([product * maps[16:24], product * maps[8:16]], axis=0)
                )
            )
        f1, f2, f3, f4 = flows
        a, b, c, d = f1 + f4, f2 + f3, f1 - f4, f3 - f2
        for cls, total in enumerate((a + b, a - b, c + d, c - d)):
            high = total.astype(BF16)
            flow[cls, :, k : k + 128] = jnp.concatenate(
                [high, (total - high.astype(F32)).astype(BF16)], axis=0
            )

    tilts = jnp.cos(angle_ref[...][None, :])
    place = lax.broadcasted_iota(jnp.int32, tilts.shape, 1) - lax.axis_index(BLK) * cycles
    tilt = [
        jnp.sum(jnp.where(place == i, tilts, 0.0), axis=1, keepdims=True) for i in range(cycles)
    ]
    tilt = jnp.where(lax.broadcasted_iota(jnp.int32, (8, 1), 0) < 4, tilt[0], tilt[1])
    for cls in range(4):
        both = lax.dot_general(
            flow[cls], table[cls], (((1,), (1,)), ((), ())), preferred_element_type=F32
        )
        mode = rounded((both[0:16] + both[16:32]) * scale)
        tilted = rounded(tilt * mode[0:8])
        parts = []
        for cycle in range(2):
            for rows in (tilted, mode[0:8], mode[8:16]):
                parts.append(jnp.sum(rows[4 * cycle : 4 * cycle + 4], axis=0, keepdims=True))
            parts.append(jnp.zeros_like(parts[0]))
        tot_ref[:, cls * depth : (cls + 1) * depth] = jnp.concatenate(parts, axis=0).astype(BF16)
        for p in range(2):
            for pair in range(half // 2):
                start = p * 4 * per_class + cls * per_class + 8 * pair
                rows_ref[start : start + 8, :] = block_swap(
                    mode[8 * p : 8 * p + 8, 128 * pair : 128 * pair + 128]
                )
    pack(rows_ref, own_ref, spread, 0)


def pack(rows_ref, out_ref, spread, first_column):
    blocks = out_ref.shape[0]
    for k in range(rows_ref.shape[0] // 128):
        tile = rows_ref[128 * k : 128 * k + 128, :].T
        spread[k, pl.ds(0, blocks, stride=2), :] = tile[0:blocks]
        spread[k, pl.ds(1, blocks, stride=2), :] = tile[blocks:]
        column = first_column + 128 * k
        out_ref[:, :, column : column + 128] = spread[k].reshape(blocks, 2, 128).astype(BF16)


def pack_totals(own_ref, mine_ref, near_ref, far_ref, near_far_ref, out_ref, spread, rows_ref):
    pairs = mine_ref.shape[1] // 128
    own_width = own_ref.shape[2]
    out_ref[:, :, :own_width] = own_ref[...]
    parts = (mine_ref, near_ref, far_ref, near_far_ref)
    total = sum(part[...].astype(F32) for part in parts)
    high = rounded(total)
    low = total - high
    for n, source in enumerate((high, low)):
        for pair in range(pairs):
            start = 8 * (n * pairs + pair)
            rows_ref[start : start + 8, :] = block_swap(source[:, 128 * pair : 128 * pair + 128])
    pack(rows_ref, out_ref, spread, own_width)


def estimate_sums(
    z_ref, leg_hbm, lad_ref, angle_ref, lead_ref,
    field_ref, power_ref,
    leg_ref, rows_ref, auto_ref, cross_ref, share_ref, leg_sems,
    *, sim_total,
):
    orders, length = leg_ref.shape[:2]
    for n in range(1, AHEAD + 1):
        fetch(leg_hbm, leg_ref, leg_sems, n).start()
    per_class = 2 * orders
    degree = lax.broadcasted_iota(jnp.int32, (1, length), 1).astype(F32)
    row = lax.broadcasted_iota(jnp.int32, (8, 1), 0)
    sign = jnp.where(row < 4, 1.0, -1.0)
    share = field_ref.shape[2]
    here = pl.ds(pl.multiple_of(lax.axis_index("sims") * share, 128), share)
    first = first_order(orders)
    tilt = jnp.cos(angle_ref[...][None, :])
    for k in range(z_ref.shape[2] // 128):
        columns = slice(128 * k, 128 * k + 128)
        rows_ref[columns, :] = z_ref[:, :, columns].astype(F32).reshape(-1, 128).T
    auto_ref[...] = jnp.zeros_like(auto_ref)
    cross_ref[...] = jnp.zeros_like(cross_ref)

    def some(step, values):
        start = pl.multiple_of(step * STEP, STEP)


        def piece(p, cls):
            place = p * 4 * per_class + cls * per_class + 8 * step
            return rows_ref[pl.ds(pl.multiple_of(place, 8), 8), :]

        pieces = [[piece(p, cls) for cls in range(4)] for p in range(4)]
        auto = auto_ref[...]
        cross = cross_ref[...]
        for i in range(STEP):
            par, h = i % 2, 4 * (i // 2)
            order = (first + start + i).astype(F32)

            def own(p):
                return jnp.concatenate(
                    [pieces[p][par][h : h + 4], pieces[p][2 + par][h : h + 4]], axis=0
                )

            def whole(p, k):
                return jnp.where(
                    row < 4,
                    pieces[p][par][h + k : h + k + 1],
                    pieces[p][2 + par][h + k : h + k + 1],
                )

            first_mode, second_mode = own(0), own(1)
            stacked = jnp.concatenate(
                [rounded(tilt * first_mode), first_mode, second_mode]
                + [whole(p, k) for p in (2, 3) for k in range(3)],
                axis=0,
            ).astype(BF16)
            projected = lax.dot_general(
                stacked, values(start, i), (((1,), (1,)), ((), ())), preferred_element_type=F32
            )
            steps = lad_ref[pl.ds(start + i, 1), :]

            def combine(zero, one, two):
                return (
                    degree * zero - steps * turned(one, 1, 1) + (order * sign) * turned(two, 4, 0)
                ) * (1.0 / length)

            estimate = combine(projected[0:8], projected[8:16], projected[16:24])
            field = combine(
                projected[24:32] + projected[48:56],
                projected[32:40] + projected[56:64],
                projected[40:48] + projected[64:72],
            )
            share_ref[i] = field
            mine = share_ref[i, :, here]
            field_ref[start + i] = jnp.concatenate([mine[0:1], mine[4:5]], axis=0)
            residual = estimate - field * (1.0 / sim_total)
            partner = jnp.where(row % 2 == 0, turned(residual, -1, 0), turned(residual, 1, 0))
            doubled = jnp.where(order > 0, 2.0, 1.0) * residual
            auto = auto + doubled * residual
            cross = cross + doubled * partner
        auto_ref[...] = auto
        cross_ref[...] = cross

    def later(step, carry):
        fetch(leg_hbm, leg_ref, leg_sems, step).wait()

        @pl.when(step + AHEAD < orders // STEP)
        def _():
            fetch(leg_hbm, leg_ref, leg_sems, step + AHEAD).start()

        some(step, lambda start, i: leg_ref[start + i])
        return carry

    some(0, lambda start, i: lead_ref[i])
    lax.fori_loop(1, orders // STEP, later, 0)
    auto = auto_ref[0:4, :] + auto_ref[4:8, :]
    cross = cross_ref[0:4, :] + cross_ref[4:8, :]
    for s in range(4):
        power_ref[s] = jnp.concatenate([auto[s : s + 1], cross[s : s + 1]], axis=0)


def exchanged(array, axis, shift=None, flip=None):
    size = lax.axis_size(axis)
    pairs = [(i, i ^ flip if flip else (i + shift) % size) for i in range(size)]
    return lax.ppermute(array, axis, pairs)


def per_device(sim_alm, t_filter, wiener_filter, colatitude, legendre, pixel_mask):
    orders, sims_here, _, length = sim_alm.shape
    cycles = legendre.shape[2]
    pixels = pixel_mask.shape[1]
    blocks = lax.axis_size(BLK)
    sim_groups = lax.axis_size("sims")
    local_cycles = cycles // blocks
    grid = orders // STEP
    degree = jnp.arange(length, dtype=F32)
    outside = pl.BlockSpec(memory_space=pl.ANY)
    inside = pl.BlockSpec(memory_space=pltpu.VMEM)

    wide = -(-3 * 8 * orders // 128) * 128
    coefs = pl.pallas_call(
        legendre_sums,
        in_specs=[outside] * 5,
        out_specs=inside,
        out_shape=jax.ShapeDtypeStruct((blocks, local_cycles, wide), BF16),
        scratch_shapes=[
            pltpu.VMEM(sim_alm.shape, BF16),
            pltpu.VMEM(legendre.shape, BF16),
            pltpu.VMEM((length,), F32),
            pltpu.VMEM((length,), F32),
            pltpu.VMEM((cycles,), F32),
            pltpu.VMEM((orders, length), F32),
            pltpu.VMEM((STEP, 32, cycles), F32),
            pltpu.VMEM((wide, cycles), F32),
            pltpu.SemaphoreType.DMA((4,)),
            pltpu.SemaphoreType.DMA((grid,)),
        ],
        name="legendre_sums",
    )(sim_alm, legendre, t_filter, wiener_filter, colatitude)
    arrived = lax.all_to_all(coefs, BLK, 0, 0, tiled=True)

    fold = pixels // 4
    width = -(-(fold + 1) // 128) * 128
    span = 2 * orders * blocks
    pixel_ids = np.arange(width)
    coarse = 2.0 * np.pi / pixels * (orders * np.arange(blocks)[:, None] * pixel_ids % pixels)
    fine = 2.0 * np.pi / pixels * (np.arange(orders)[:, None] * pixel_ids % pixels)
    turns = np.concatenate(
        [np.cos(coarse), -np.sin(coarse), np.cos(fine), -np.sin(fine)]
    ).astype(np.float32)
    half_table = (2, span // 4, width)
    table, steps, quarters, lead = pl.pallas_call(
        make_table,
        in_specs=[inside, inside, outside],
        out_specs=[outside, inside, inside, inside],
        out_shape=[
            jax.ShapeDtypeStruct(half_table, BF16),
            jax.ShapeDtypeStruct((orders, length), F32),
            jax.ShapeDtypeStruct((4 * local_cycles, width), F32),
            jax.ShapeDtypeStruct((STEP, length, cycles), BF16),
        ],
        scratch_shapes=[
            pltpu.VMEM(half_table, BF16),
            pltpu.SemaphoreType.DMA((orders // 2, 2)),
            pltpu.SemaphoreType.DMA,
        ],
        cost_estimate=pl.CostEstimate(
            flops=3 * span * width, bytes_accessed=span * width, transcendentals=0
        ),
        compiler_params=ROOM,
        name="make_table",
    )(
        turns,
        pixel_mask,
        legendre,
    )

    own, partial_total = pl.pallas_call(
        functools.partial(fourier_sums, scale=2.0 * math.pi / pixels, orders=orders),
        in_specs=[inside, outside] + [inside] * 3,
        out_shape=[
            jax.ShapeDtypeStruct((blocks, local_cycles, 16 * orders), BF16),
            jax.ShapeDtypeStruct((8, span), BF16),
        ],
        scratch_shapes=[
            pltpu.VMEM((4, span // 4, width), BF16),
            pltpu.VMEM((24, span), BF16),
            pltpu.VMEM((wide // 128, cycles, 128), F32),
            pltpu.VMEM((4, 24, width), F32),
            pltpu.VMEM((4, 32, width), BF16),
            pltpu.VMEM((16 * orders, cycles), F32),
            pltpu.SemaphoreType.DMA((2,)),
        ],
        compiler_params=ROOM,
        name="fourier_sums",
    )(arrived, table, quarters, colatitude, turns)

    far = exchanged(partial_total, "sims", flip=2)
    near = exchanged(partial_total, "sims", flip=1)
    near_far = exchanged(far, "sims", flip=1)
    packed = pl.pallas_call(
        pack_totals,
        out_shape=jax.ShapeDtypeStruct((blocks, local_cycles, 32 * orders), BF16),
        scratch_shapes=[
            pltpu.VMEM((orders // 8, cycles, 128), F32),
            pltpu.VMEM((16 * orders, cycles), F32),
        ],
        compiler_params=ROOM,
        name="pack_totals",
    )(own, partial_total, near, far, near_far)
    returned = lax.all_to_all(packed, BLK, 0, 0, tiled=True)

    field_share, power = pl.pallas_call(
        functools.partial(estimate_sums, sim_total=sims_here * sim_groups),
        in_specs=[inside, outside, inside, inside, inside],
        out_shape=[
            jax.ShapeDtypeStruct((orders, 2, length // sim_groups), F32),
            jax.ShapeDtypeStruct((sims_here, 2, length), F32),
        ],
        scratch_shapes=[
            pltpu.VMEM(legendre.shape, BF16),
            pltpu.VMEM((32 * orders, cycles), F32),
            pltpu.VMEM((8, length), F32),
            pltpu.VMEM((8, length), F32),
            pltpu.VMEM((STEP, 8, length), F32),
            pltpu.SemaphoreType.DMA((grid,)),
        ],
        compiler_params=ROOM,
        name="estimate_sums",
    )(returned, legendre, steps, colatitude, lead)

    for axis in BLK:
        others = [exchanged(power, axis, shift=k) for k in range(1, lax.axis_size(axis))]
        power = power + sum(others)
    return (field_share, power / (2.0 * degree + 1.0))


def solution(mesh):
    torus = Mesh(
        mesh.devices.reshape(mesh.shape["sims"], 4, 4, 4), ("sims", "blk_0", "blk_1", "blk_2")
    )
    return jax.shard_map(
        per_device,
        mesh=torus,
        in_specs=(P(BLK, "sims", None, None), P(), P(), P(), P(BLK, None, None), P(BLK, None)),
        out_specs=(P(BLK, None, "sims"), P("sims", None, None)),
        check_vma=False,
    )
```

```python
import functools
import math

import jax
import jax.numpy as jnp
import numpy as np
from jax import lax
from jax.experimental import pallas as pl
from jax.experimental.pallas import tpu as pltpu
from jax.sharding import Mesh
from jax.sharding import PartitionSpec as P

BLK = ("blk_0", "blk_1", "blk_2")
F32 = jnp.float32
BF16 = jnp.bfloat16
ROOM = pltpu.CompilerParams(vmem_limit_bytes=52 << 20)
AHEAD = 5
STEP = 4


def ladder(degree, orders):
    numerator = (2.0 * degree + 1.0) * (degree * degree - orders * orders)
    denominator = jnp.maximum(2.0 * degree - 1.0, 1.0)
    return jnp.where(degree > orders, jnp.sqrt(jnp.maximum(numerator, 0.0) / denominator), 0.0)


def rounded(x):
    return x.astype(BF16).astype(F32)


def turned(x, shift, axis):
    return pltpu.roll(x, shift % x.shape[axis], axis)


def block_swap(x):
    row = lax.broadcasted_iota(jnp.int32, x.shape, 0) < 4
    lane = lax.broadcasted_iota(jnp.int32, x.shape, 1) < 64
    return jnp.where(row == lane, x, turned(turned(x, 64, 1), 4, 0))


def fetch(source, target, sems, n):
    rows = pl.ds(pl.multiple_of(n * STEP, STEP), STEP)
    return pltpu.make_async_copy(source.at[rows], target.at[rows], sems.at[n])


def copies(sources, targets, sems):
    return [
        pltpu.make_async_copy(source, target, sems.at[n])
        for n, (source, target) in enumerate(zip(sources, targets))
    ]


def first_order(orders):
    return lax.axis_index(BLK) * orders


def ladder_rows(orders, length):
    degree = lax.broadcasted_iota(jnp.int32, (orders, length), 1).astype(F32)
    order = (first_order(orders) + lax.broadcasted_iota(jnp.int32, (orders, length), 0)).astype(F32)
    return ladder(degree, order)


def legendre_sums(
    x_hbm, leg_hbm, t_hbm, w_hbm, angle_hbm,
    out_ref,
    x_ref, leg_ref, t_ref, w_ref, angle_ref, lad_ref, sums_ref, rows_ref, small_sems, leg_sems,
):
    orders, length = leg_ref.shape[:2]
    small = copies(
        (angle_hbm, t_hbm, w_hbm, x_hbm), (angle_ref, t_ref, w_ref, x_ref), small_sems
    )
    for copy in small + [fetch(leg_hbm, leg_ref, leg_sems, 0)]:
        copy.start()

    lad_ref[...] = ladder_rows(orders, length)
    rows_ref[...] = jnp.zeros_like(rows_ref)
    degree = lax.broadcasted_iota(jnp.int32, (1, length), 1).astype(F32)
    first_half = lax.broadcasted_iota(jnp.int32, (8, 1), 0) < 4
    first = first_order(orders)
    per_class = 2 * orders
    for copy in small:
        copy.wait()
    for n in range(1, AHEAD):
        fetch(leg_hbm, leg_ref, leg_sems, n).start()
    angle = angle_ref[...][None, :]
    cosecant = 1.0 / jnp.sin(angle)
    cotangent = jnp.cos(angle) / jnp.sin(angle)
    t_row = t_ref[...][None, :]
    w_row = w_ref[...][None, :]

    def some(step, carry):
        start = pl.multiple_of(step * STEP, STEP)
        fetch(leg_hbm, leg_ref, leg_sems, step).wait()

        @pl.when(step + AHEAD < orders // STEP)
        def _():
            fetch(leg_hbm, leg_ref, leg_sems, step + AHEAD).start()

        for i in range(STEP):
            values = x_ref[start + i].astype(F32).reshape(8, length)
            weighted = w_row * values
            raised = lad_ref[pl.ds(start + i, 1), :] * weighted
            coefs = jnp.concatenate(
                [t_row * values, weighted, degree * weighted, turned(raised, -1, 1)], axis=0
            ).astype(BF16)
            sums_ref[i] = jnp.dot(coefs, leg_ref[start + i], preferred_element_type=F32)
        for par in range(2):

            def pair(k, c):
                return jnp.concatenate(
                    [sums_ref[i, pl.ds(8 * k + c, 4, stride=2), :] for i in (par, par + 2)], axis=0
                )

            order = jnp.where(first_half, first + start + par, first + start + par + 2)
            spin = order.astype(F32) * cosecant
            for c in range(2):
                spun = pair(1, 1 - c) * spin
                slopes = cotangent * pair(2, c) - cosecant * pair(3, c)
                for q, rows in enumerate((pair(0, c), spun if c else -spun, slopes)):
                    place = q * 4 * per_class + (2 * c + par) * per_class
                    rows_ref[pl.ds(pl.multiple_of(place + 8 * step, 8), 8), :] = rows
        return carry

    lax.fori_loop(0, orders // STEP, some, 0)
    for k in range(rows_ref.shape[0] // 128):
        columns = slice(128 * k, 128 * k + 128)
        out_ref[:, :, columns] = rows_ref[columns, :].T.reshape(-1, 2, 128).astype(BF16)


def table_rows(turns, blocks, order, cosines, sines, rows):
    orders = turns.shape[0] // 2 - blocks
    cb_row = turns[pl.ds(2 * blocks + order, 1), :]
    sb_row = turns[pl.ds(2 * blocks + orders + order, 1), :]
    for k in range(0, turns.shape[1], 128):
        columns = slice(k, k + 128)
        ca = turns[:blocks, columns]
        sa = turns[blocks : 2 * blocks, columns]
        cb = cb_row[:, columns]
        sb = sb_row[:, columns]
        cosines[rows, columns] = (ca * cb - sa * sb).astype(BF16)
        sines[rows, columns] = (sa * cb + ca * sb).astype(BF16)


def make_table(
    turns, pixel_ref, leg_hbm,
    table_hbm, lad_ref, quarter_ref, lead_ref,
    table, sems, lead_sem,
):
    lead = pltpu.make_async_copy(leg_hbm.at[pl.ds(0, STEP)], lead_ref, lead_sem)
    lead.start()
    width = turns.shape[1]
    orders = lad_ref.shape[0]
    blocks = turns.shape[0] // 2 - orders

    def stores(h):
        rows = pl.ds(pl.multiple_of(h * blocks, blocks), blocks)
        return [
            pltpu.make_async_copy(table.at[c, rows], table_hbm.at[c, rows], sems.at[h, c])
            for c in range(2)
        ]

    def turn(h, carry):
        rows = pl.ds(pl.multiple_of(h * blocks, blocks), blocks)
        table_rows(turns, blocks, 2 * h, table.at[0], table.at[1], rows)
        for copy in stores(h):
            copy.start()
        return carry

    lax.fori_loop(0, orders // 2, turn, 0)

    lad_ref[...] = ladder_rows(orders, lad_ref.shape[1])

    fold = pixel_ref.shape[1] // 4
    weight = pixel_ref[...].astype(F32)
    cycles = weight.shape[0]
    end = jnp.zeros((cycles, width - fold), F32)
    lane = lax.broadcasted_iota(jnp.int32, (cycles, width), 1)
    row = lax.broadcasted_iota(jnp.int32, (128, 128), 0)
    column = lax.broadcasted_iota(jnp.int32, (128, 128), 1)
    flip = jnp.where(row + column == 127, 1.0, 0.0).astype(BF16)
    for n in range(2):
        near = weight[:, 2 * n * fold : (2 * n + 1) * fold]
        far = weight[:, (2 * n + 1) * fold : (2 * n + 2) * fold]
        flipped = jnp.concatenate(
            [
                jnp.dot(far[:, k : k + 128].astype(BF16), flip, preferred_element_type=F32)
                for k in range(fold - 128, -1, -128)
            ],
            axis=1,
        )
        first = jnp.concatenate([near, end], axis=1)
        second = jnp.concatenate([turned(flipped, 1, 1), end], axis=1)
        quarter_ref[4 * n : 4 * n + 2, :] = jnp.where(lane == fold, turned_edge(far, lane), first)
        quarter_ref[4 * n + 2 : 4 * n + 4, :] = jnp.where(lane == 0, 0.0, second)

    def finish(h, carry):
        for copy in stores(h):
            copy.wait()
        return carry

    lax.fori_loop(0, orders // 2, finish, 0)
    lead.wait()


def turned_edge(far, lane):
    return jnp.broadcast_to(far[:, 0:1], lane.shape)


def fourier_sums(
    y_ref, table_hbm, mask_ref, angle_ref, turns,
    own_ref, tot_ref,
    table, lhs, spread, acc, flow, rows_ref, table_sems,
    *, scale, orders,
):
    blocks, cycles = y_ref.shape[:2]
    half = orders // 2
    per_class = 2 * orders
    depth = half * blocks
    width = table.shape[2]
    loads = [
        pltpu.make_async_copy(table_hbm.at[c], table.at[2 * c], table_sems.at[c]) for c in range(2)
    ]
    for copy in loads:
        copy.start()

    arrived = []
    for k in range(y_ref.shape[2] // 128):
        spread[k] = y_ref[:, :, 128 * k : 128 * k + 128].astype(F32).reshape(-1, 128)
        parts = [spread[k, pl.ds(i, blocks, stride=2), :] for i in range(2)]
        arrived.append(jnp.concatenate(parts, axis=0).T)
    turned_rows = jnp.concatenate(arrived, axis=0)
    lane = lax.broadcasted_iota(jnp.int32, (8, 128), 1)
    for cls in range(4):
        for pair in range(half // 2):
            tiles = []
            for q in range(3):
                start = q * 4 * per_class + cls * per_class + 8 * pair
                tile = block_swap(turned_rows[start : start + 8])
                if cls % 2 == 0 and pair == 0:
                    tiles.append(jnp.where(lane == 0, tile, tile * 2.0))
                else:
                    tiles.append(tile * 2.0)
            column = cls * depth + 128 * pair
            lhs[:, column : column + 128] = jnp.concatenate(tiles, axis=0).astype(BF16)

    def turn(h, carry):
        rows = pl.ds(pl.multiple_of(h * blocks, blocks), blocks)
        table_rows(turns, blocks, 2 * h + 1, table.at[1], table.at[3], rows)
        return carry

    lax.fori_loop(0, half, turn, 0)
    for cls in (1, 3, 0, 2):
        if cls % 2 == 0:
            loads[cls // 2].wait()
        acc[cls] = jnp.dot(
            lhs[:, cls * depth : (cls + 1) * depth], table[cls], preferred_element_type=F32
        )

    first_cycle = lax.broadcasted_iota(jnp.int32, (8, 128), 0) < 4
    for k in range(0, width, 128):
        ee, eo, oe, oo = (acc[cls, :, k : k + 128] for cls in range(4))
        x, u, y, v = ee + eo, ee - eo, oe + oo, oe - oo
        flows = []
        for quarter, maps in enumerate((x + y, u - v, u + v, x - y)):
            weight = jnp.where(
                first_cycle,
                mask_ref[2 * quarter : 2 * quarter + 1, k : k + 128],
                mask_ref[2 * quarter + 1 : 2 * quarter + 2, k : k + 128],
            )
            product = weight * maps[0:8]
            flows.append(
                rounded(
                    jnp.concatenate([product * maps[16:24], product * maps[8:16]], axis=0)
                )
            )
        f1, f2, f3, f4 = flows
        a, b, c, d = f1 + f4, f2 + f3, f1 - f4, f3 - f2
        for cls, total in enumerate((a + b, a - b, c + d, c - d)):
            high = total.astype(BF16)
            flow[cls, :, k : k + 128] = jnp.concatenate(
                [high, (total - high.astype(F32)).astype(BF16)], axis=0
            )

    tilts = jnp.cos(angle_ref[...][None, :])
    place = lax.broadcasted_iota(jnp.int32, tilts.shape, 1) - lax.axis_index(BLK) * cycles
    tilt = [
        jnp.sum(jnp.where(place == i, tilts, 0.0), axis=1, keepdims=True) for i in range(cycles)
    ]
    tilt = jnp.where(lax.broadcasted_iota(jnp.int32, (8, 1), 0) < 4, tilt[0], tilt[1])
    for cls in range(4):
        both = lax.dot_general(
            flow[cls], table[cls], (((1,), (1,)), ((), ())), preferred_element_type=F32
        )
        mode = rounded((both[0:16] + both[16:32]) * scale)
        tilted = rounded(tilt * mode[0:8])
        parts = []
        for cycle in range(2):
            for rows in (tilted, mode[0:8], mode[8:16]):
                parts.append(jnp.sum(rows[4 * cycle : 4 * cycle + 4], axis=0, keepdims=True))
            parts.append(jnp.zeros_like(parts[0]))
        tot_ref[:, cls * depth : (cls + 1) * depth] = jnp.concatenate(parts, axis=0)
        for p in range(2):
            for pair in range(half // 2):
                start = p * 4 * per_class + cls * per_class + 8 * pair
                rows_ref[start : start + 8, :] = block_swap(
                    mode[8 * p : 8 * p + 8, 128 * pair : 128 * pair + 128]
                )
    pack(rows_ref, own_ref, spread, 0)


def pack(rows_ref, out_ref, spread, first_column):
    blocks = out_ref.shape[0]
    for k in range(rows_ref.shape[0] // 128):
        tile = rows_ref[128 * k : 128 * k + 128, :].T
        spread[k, pl.ds(0, blocks, stride=2), :] = tile[0:blocks]
        spread[k, pl.ds(1, blocks, stride=2), :] = tile[blocks:]
        column = first_column + 128 * k
        out_ref[:, :, column : column + 128] = spread[k].reshape(blocks, 2, 128).astype(BF16)


def pack_totals(own_ref, mine_ref, far_ref, out_ref, spread, rows_ref):
    pairs = mine_ref.shape[1] // 128
    own_width = own_ref.shape[2]
    out_ref[:, :, :own_width] = own_ref[...]
    parts = (mine_ref, far_ref)
    total = sum(part[...].astype(F32) for part in parts)
    high = rounded(total)
    low = total - high
    for n, source in enumerate((high, low)):
        for pair in range(pairs):
            start = 8 * (n * pairs + pair)
            rows_ref[start : start + 8, :] = block_swap(source[:, 128 * pair : 128 * pair + 128])
    pack(rows_ref, out_ref, spread, own_width)


def estimate_sums(
    z_ref, leg_hbm, lad_ref, angle_ref, lead_ref,
    field_ref, power_ref,
    leg_ref, rows_ref, auto_ref, cross_ref, share_ref, leg_sems,
    *, sim_total,
):
    orders, length = leg_ref.shape[:2]
    for n in range(1, AHEAD + 1):
        fetch(leg_hbm, leg_ref, leg_sems, n).start()
    per_class = 2 * orders
    degree = lax.broadcasted_iota(jnp.int32, (1, length), 1).astype(F32)
    row = lax.broadcasted_iota(jnp.int32, (8, 1), 0)
    sign = jnp.where(row < 4, 1.0, -1.0)
    share = field_ref.shape[2]
    here = pl.ds(pl.multiple_of(lax.axis_index("sims") * share, 128), share)
    first = first_order(orders)
    tilt = jnp.cos(angle_ref[...][None, :])
    for k in range(z_ref.shape[2] // 128):
        columns = slice(128 * k, 128 * k + 128)
        rows_ref[columns, :] = z_ref[:, :, columns].astype(F32).reshape(-1, 128).T
    auto_ref[...] = jnp.zeros_like(auto_ref)
    cross_ref[...] = jnp.zeros_like(cross_ref)

    def some(step, values):
        start = pl.multiple_of(step * STEP, STEP)


        def piece(p, cls):
            place = p * 4 * per_class + cls * per_class + 8 * step
            return rows_ref[pl.ds(pl.multiple_of(place, 8), 8), :]

        pieces = [[piece(p, cls) for cls in range(4)] for p in range(4)]
        auto = auto_ref[...]
        cross = cross_ref[...]
        for i in range(STEP):
            par, h = i % 2, 4 * (i // 2)
            order = (first + start + i).astype(F32)

            def own(p):
                return jnp.concatenate(
                    [pieces[p][par][h : h + 4], pieces[p][2 + par][h : h + 4]], axis=0
                )

            def whole(p, k):
                return jnp.where(
                    row < 4,
                    pieces[p][par][h + k : h + k + 1],
                    pieces[p][2 + par][h + k : h + k + 1],
                )

            first_mode, second_mode = own(0), own(1)
            stacked = jnp.concatenate(
                [rounded(tilt * first_mode), first_mode, second_mode]
                + [whole(p, k) for p in (2, 3) for k in range(3)],
                axis=0,
            ).astype(BF16)
            projected = lax.dot_general(
                stacked, values(start, i), (((1,), (1,)), ((), ())), preferred_element_type=F32
            )
            steps = lad_ref[pl.ds(start + i, 1), :]

            def combine(zero, one, two):
                return (
                    degree * zero - steps * turned(one, 1, 1) + (order * sign) * turned(two, 4, 0)
                ) * (1.0 / length)

            estimate = combine(projected[0:8], projected[8:16], projected[16:24])
            field = combine(
                projected[24:32] + projected[48:56],
                projected[32:40] + projected[56:64],
                projected[40:48] + projected[64:72],
            )
            share_ref[i] = field
            mine = share_ref[i, :, here]
            field_ref[start + i] = jnp.concatenate([mine[0:1], mine[4:5]], axis=0)
            residual = estimate - field * (1.0 / sim_total)
            partner = jnp.where(row % 2 == 0, turned(residual, -1, 0), turned(residual, 1, 0))
            doubled = jnp.where(order > 0, 2.0, 1.0) * residual
            auto = auto + doubled * residual
            cross = cross + doubled * partner
        auto_ref[...] = auto
        cross_ref[...] = cross

    def later(step, carry):
        fetch(leg_hbm, leg_ref, leg_sems, step).wait()

        @pl.when(step + AHEAD < orders // STEP)
        def _():
            fetch(leg_hbm, leg_ref, leg_sems, step + AHEAD).start()

        some(step, lambda start, i: leg_ref[start + i])
        return carry

    some(0, lambda start, i: lead_ref[i])
    lax.fori_loop(1, orders // STEP, later, 0)
    auto = auto_ref[0:4, :] + auto_ref[4:8, :]
    cross = cross_ref[0:4, :] + cross_ref[4:8, :]
    for s in range(4):
        power_ref[s] = jnp.concatenate([auto[s : s + 1], cross[s : s + 1]], axis=0)


def exchanged(array, axis, flip):
    return lax.ppermute(array, axis, [(i, i ^ flip) for i in range(lax.axis_size(axis))])


def per_device(sim_alm, t_filter, wiener_filter, colatitude, legendre, pixel_mask):
    orders, sims_here, _, length = sim_alm.shape
    cycles = legendre.shape[2]
    pixels = pixel_mask.shape[1]
    blocks = lax.axis_size(BLK)
    sim_groups = lax.axis_size("sims")
    local_cycles = cycles // blocks
    grid = orders // STEP
    degree = jnp.arange(length, dtype=F32)
    outside = pl.BlockSpec(memory_space=pl.ANY)
    inside = pl.BlockSpec(memory_space=pltpu.VMEM)

    wide = -(-3 * 8 * orders // 128) * 128
    coefs = pl.pallas_call(
        legendre_sums,
        in_specs=[outside] * 5,
        out_specs=inside,
        out_shape=jax.ShapeDtypeStruct((blocks, local_cycles, wide), BF16),
        scratch_shapes=[
            pltpu.VMEM(sim_alm.shape, BF16),
            pltpu.VMEM(legendre.shape, BF16),
            pltpu.VMEM((length,), F32),
            pltpu.VMEM((length,), F32),
            pltpu.VMEM((cycles,), F32),
            pltpu.VMEM((orders, length), F32),
            pltpu.VMEM((STEP, 32, cycles), F32),
            pltpu.VMEM((wide, cycles), F32),
            pltpu.SemaphoreType.DMA((4,)),
            pltpu.SemaphoreType.DMA((grid,)),
        ],
        name="legendre_sums",
    )(sim_alm, legendre, t_filter, wiener_filter, colatitude)
    arrived = lax.all_to_all(coefs, BLK, 0, 0, tiled=True)

    fold = pixels // 4
    width = -(-(fold + 1) // 128) * 128
    span = 2 * orders * blocks
    pixel_ids = np.arange(width)
    coarse = 2.0 * np.pi / pixels * (orders * np.arange(blocks)[:, None] * pixel_ids % pixels)
    fine = 2.0 * np.pi / pixels * (np.arange(orders)[:, None] * pixel_ids % pixels)
    turns = np.concatenate(
        [np.cos(coarse), -np.sin(coarse), np.cos(fine), -np.sin(fine)]
    ).astype(np.float32)
    half_table = (2, span // 4, width)
    table, steps, quarters, lead = pl.pallas_call(
        make_table,
        in_specs=[inside, inside, outside],
        out_specs=[outside, inside, inside, inside],
        out_shape=[
            jax.ShapeDtypeStruct(half_table, BF16),
            jax.ShapeDtypeStruct((orders, length), F32),
            jax.ShapeDtypeStruct((4 * local_cycles, width), F32),
            jax.ShapeDtypeStruct((STEP, length, cycles), BF16),
        ],
        scratch_shapes=[
            pltpu.VMEM(half_table, BF16),
            pltpu.SemaphoreType.DMA((orders // 2, 2)),
            pltpu.SemaphoreType.DMA,
        ],
        cost_estimate=pl.CostEstimate(
            flops=3 * span * width, bytes_accessed=span * width, transcendentals=0
        ),
        compiler_params=ROOM,
        name="make_table",
    )(
        turns,
        pixel_mask,
        legendre,
    )

    own, partial_total = pl.pallas_call(
        functools.partial(fourier_sums, scale=2.0 * math.pi / pixels, orders=orders),
        in_specs=[inside, outside] + [inside] * 3,
        out_shape=[
            jax.ShapeDtypeStruct((blocks, local_cycles, 16 * orders), BF16),
            jax.ShapeDtypeStruct((8, span), F32),
        ],
        scratch_shapes=[
            pltpu.VMEM((4, span // 4, width), BF16),
            pltpu.VMEM((24, span), BF16),
            pltpu.VMEM((wide // 128, cycles, 128), F32),
            pltpu.VMEM((4, 24, width), F32),
            pltpu.VMEM((4, 32, width), BF16),
            pltpu.VMEM((16 * orders, cycles), F32),
            pltpu.SemaphoreType.DMA((2,)),
        ],
        compiler_params=ROOM,
        name="fourier_sums",
    )(arrived, table, quarters, colatitude, turns)

    chip_total = partial_total + exchanged(partial_total, "sims", flip=1)
    chip_total = chip_total.astype(BF16)
    far = exchanged(chip_total, "sims", flip=2)
    packed = pl.pallas_call(
        pack_totals,
        out_shape=jax.ShapeDtypeStruct((blocks, local_cycles, 32 * orders), BF16),
        scratch_shapes=[
            pltpu.VMEM((orders // 8, cycles, 128), F32),
            pltpu.VMEM((16 * orders, cycles), F32),
        ],
        compiler_params=ROOM,
        name="pack_totals",
    )(own, chip_total, far)
    returned = lax.all_to_all(packed, BLK, 0, 0, tiled=True)

    field_share, power = pl.pallas_call(
        functools.partial(estimate_sums, sim_total=sims_here * sim_groups),
        in_specs=[inside, outside, inside, inside, inside],
        out_shape=[
            jax.ShapeDtypeStruct((orders, 2, length // sim_groups), F32),
            jax.ShapeDtypeStruct((sims_here, 2, length), F32),
        ],
        scratch_shapes=[
            pltpu.VMEM(legendre.shape, BF16),
            pltpu.VMEM((32 * orders, cycles), F32),
            pltpu.VMEM((8, length), F32),
            pltpu.VMEM((8, length), F32),
            pltpu.VMEM((STEP, 8, length), F32),
            pltpu.SemaphoreType.DMA((grid,)),
        ],
        compiler_params=ROOM,
        name="estimate_sums",
    )(returned, legendre, steps, colatitude, lead)

    for axis in (BLK[1], BLK[0], BLK[2]):
        others = [exchanged(power, axis, flip=k) for k in range(1, lax.axis_size(axis))]
        power = power + sum(others)
    return (field_share, power / (2.0 * degree + 1.0))


def solution(mesh):
    torus = Mesh(
        mesh.devices.reshape(mesh.shape["sims"], 4, 4, 4), ("sims", "blk_0", "blk_1", "blk_2")
    )
    return jax.shard_map(
        per_device,
        mesh=torus,
        in_specs=(P(BLK, "sims", None, None), P(), P(), P(), P(BLK, None, None), P(BLK, None)),
        out_specs=(P(BLK, None, "sims"), P("sims", None, None)),
        check_vma=False,
    )
```
